256 devices in a mesh: seq: 64 (over x, z, core), head: 4 (over y).
Axes of the slice: x: 4, y: 4, z: 8, core: 2. Of those that a mesh axis runs over, the one named last changes fastest.
Arguments:
- queries: bfloat16 [32768, 1024], P('seq', 'head'), may hold values from -6 to 6
- key_vectors: bfloat16 [32768, 1024], P('seq', 'head'), may hold values from -6 to 6
- values: bfloat16 [32768, 2048], P('seq', 'head'), may hold values from -6 to 6
- log_gate: bfloat16 [32768, 1024], P('seq', 'head'), may hold values from -1.6 to 0, as said below
- out_gate: bfloat16 [32768, 2048], P('seq', 'head'), may hold values from -6 to 6
- norm_gain: float32 [2048], P('head'), may hold values from 0.5 to 1.5
- out_weight: bfloat16 [2048, 2048], P('head'), may hold values from -0.1875 to 0.1875
Outputs:
- mixed: bfloat16 [32768, 2048], P('seq', 'head')
The draws below stay inside these ranges and needn't reach their ends.
Inputs may be any that keep to these rules, and one draw needn't show every extreme that they name: `log_gate`: every entry is below zero.
All inputs are finite; a program needn't handle non-finite values.
Results may differ from the reference program's by a relative error of at most 0.017.
Values may be sent and summed in bfloat16 or wider, within the bound.
A program may use at most 128 MiB of HBM per device.

```python
import jax
import jax.numpy as jnp
from jax import lax

D = 2048
H = 4
DK = 256
DV = 512
SPAN = 64
TOK_DEV = 512
SEQUENCE_TOKENS = 32768
N_HEAD = 4


def draw_log_gate(key, part):
    parallel_lanes = jax.random.split(key, 7)
    blocks_all = SEQUENCE_TOKENS // TOK_DEV
    quick_count = H // 2
    order = jax.random.permutation(parallel_lanes[0], H)
    quick_head = order < quick_count
    quick_rate = jnp.exp(jax.random.uniform(parallel_lanes[1], (H, DK), minval=jnp.log(0.02), maxval=jnp.log(0.06)))
    slow_rate = jnp.exp(jax.random.uniform(parallel_lanes[2], (H, DK), minval=jnp.log(0.05), maxval=jnp.log(0.25))) / SEQUENCE_TOKENS
    base_rate = jnp.where(quick_head[:, None], quick_rate, slow_rate).reshape(1, 1, H * DK)
    device_factor = jnp.exp(jax.random.uniform(parallel_lanes[3], (blocks_all, 1, H * DK), minval=jnp.log(0.5), maxval=jnp.log(2.0)))
    roughness = jax.random.uniform(parallel_lanes[4], (blocks_all, TOK_DEV, H * DK), minval=0.5, maxval=1.5)
    decay_factor = (base_rate * device_factor * roughness).reshape(SEQUENCE_TOKENS, H * DK)
    block_offset = jax.random.randint(parallel_lanes[5], (2,), 0, SEQUENCE_TOKENS)
    block_length = jnp.log(jax.random.uniform(parallel_lanes[6], (2,), minval=0.5, maxval=0.8))
    token_position = lax.iota(jnp.int32, SEQUENCE_TOKENS)
    token_block = jnp.sum(jnp.where(token_position[:, None] == block_offset[None, :], block_length[None, :], 0.0), axis=1)
    return (token_block[:, None] - decay_factor).astype(jnp.bfloat16)


def raised(entries, rng, source, target, parts, factor):
    def block_of(dim):
        return (jnp.arange(entries.shape[dim]) // (entries.shape[dim] // parts)).reshape((-1,) + (1,) * (entries.ndim - 1 - dim))

    near = jax.random.permutation(rng, parts)[block_of(target)]
    other_side = (block_of(target) + parts // 2) % parts
    return jnp.where((block_of(source) == near) | (block_of(source) == other_side), factor * entries, entries)


def steps_of(stream_key, dims, pieces, least, largest):
    def one(axis_at, shards_of):
        heights = jax.random.uniform(jax.random.fold_in(jax.random.fold_in(stream_key, 6), axis_at), (shards_of,), jnp.float32, least / len(pieces), largest / len(pieces))
        return jnp.repeat(jnp.exp(heights), dims[axis_at] // shards_of).reshape((-1,) + (1,) * (len(dims) - axis_at - 1))

    factor_of = one(*pieces[0])
    for cut in pieces[1:]:
        factor_of = factor_of * one(*cut)
    return factor_of


def normal_values(stream_key, shape, scale, most, cuts=(), kind=jnp.bfloat16):
    factor_of = steps_of(stream_key, shape, cuts, -0.22, 0.18) if cuts else 1.0
    result = jax.random.normal(stream_key, shape, jnp.float32) * scale * factor_of
    return jnp.minimum(jnp.maximum(result, -most), most).astype(kind)


def noise_with(own_key, dims, scale, reach, cuts, heavy, dtype=jnp.bfloat16):
    array = scale * jax.random.normal(own_key, dims, jnp.float32)
    if cuts:
        array = array * steps_of(own_key, dims, cuts, -0.22, 0.18)
    return jnp.clip(raised(array, jax.random.fold_in(own_key, 3), *heavy), -reach, reach).astype(dtype)


def setup_inputs(seed: int = 0) -> dict:
    streams_of = jax.random.split(jax.random.key(seed), 8)
    queries = normal_values(streams_of[0], (SEQUENCE_TOKENS, H * DK), 1.0, 6.0, ((0, 64), (1, 4)))
    key_vectors = normal_values(streams_of[1], (SEQUENCE_TOKENS, H * DK), 1.0, 6.0, ((0, 64), (1, 4)))
    values = normal_values(streams_of[2], (SEQUENCE_TOKENS, H * DV), 1.0, 6.0, ((0, 64), (1, 4)))
    log_gate = draw_log_gate(jax.random.fold_in(streams_of[7], 71), 0)
    out_gate = normal_values(streams_of[4], (SEQUENCE_TOKENS, H * DV), 1.0, 6.0, ((0, 64), (1, 4)))
    norm_gain = jnp.clip(1.0 + 0.1 * jax.random.normal(streams_of[5], (H * DV,), jnp.float32), 0.5, 1.5)
    out_weight = noise_with(streams_of[6], (H * DV, D), (H * DV) ** -0.5, 0.1875, ((0, 4),), (0, 1, 4, 2.0))
    return {"queries": queries, "key_vectors": key_vectors, "values": values, "log_gate": log_gate, "out_gate": out_gate, "norm_gain": norm_gain, "out_weight": out_weight}


def lowered(array_in):
    return lax.optimization_barrier(array_in.astype(jnp.bfloat16)).astype(jnp.float32)

def reference(queries, key_vectors, values, log_gate, out_gate, norm_gain, out_weight):
    blocks = SEQUENCE_TOKENS // SPAN
    middle_pos = SPAN // 2
    causal = lax.iota(jnp.int32, SPAN)[:, None] >= lax.iota(jnp.int32, SPAN)[None, :]
    gain_table = norm_gain.reshape(H, DV)

    def advance(carried, block_in):
        query_b, key_b, value_b, gate_b, outer_b = block_in
        running = jnp.cumsum(gate_b.astype(jnp.float32), axis=0)
        middle = running[middle_pos:middle_pos + 1]
        ending = running[SPAN - 1:SPAN]
        query_f = query_b.astype(jnp.float32)
        key_f = key_b.astype(jnp.float32)
        value_f = value_b.astype(jnp.float32)
        q_inter = lowered(query_f * jnp.exp(running))
        q_intra = lowered(query_f * jnp.exp(running - middle))
        k_intra = lowered(key_f * jnp.exp(middle - running))
        k_state = lowered(key_f * jnp.exp(ending - running))
        scores = jnp.einsum('thd,shd->hts', q_intra, k_intra)
        weights = lowered(jnp.where(causal[None], scores, 0.0))
        local_part = jnp.einsum('hts,she->the', weights, value_f)
        carried_low = lowered(carried)
        carried_part = jnp.einsum('thd,hed->the', q_inter, carried_low)
        attention = local_part + carried_part
        spread = lax.optimization_barrier(jnp.mean(attention * attention, axis=-1, keepdims=True))
        normed = attention / jnp.sqrt(spread + 1e-05) * gain_table
        gated_out = (normed * jax.nn.silu(outer_b.astype(jnp.float32))).astype(jnp.bfloat16)
        block_state = jnp.einsum('the,thd->hed', value_f, k_state)
        carried = carried * jnp.exp(ending[0])[:, None, :] + block_state
        return (carried, gated_out.reshape(SPAN, H * DV))
    start_state = jnp.zeros((H, DV, DK), jnp.float32)
    inputs = (queries.reshape(blocks, SPAN, H, DK), key_vectors.reshape(blocks, SPAN, H, DK), values.reshape(blocks, SPAN, H, DV), log_gate.reshape(blocks, SPAN, H, DK), out_gate.reshape(blocks, SPAN, H, DV))
    unused_state, gated_all = lax.scan(advance, start_state, inputs)
    gated_all = gated_all.reshape(SEQUENCE_TOKENS, H * DV)
    group_width = H // N_HEAD * DV
    summed = jnp.zeros((SEQUENCE_TOKENS, D), jnp.float32)
    for group_index in range(N_HEAD):
        start_row = group_index * group_width
        end_row = start_row + group_width
        partial_value = jnp.dot(gated_all[:, start_row:end_row], out_weight[start_row:end_row], preferred_element_type=jnp.float32)
        summed = summed + lowered(partial_value)
    return summed.astype(jnp.bfloat16)
```

```python
import functools

import jax
import jax.numpy as jnp
from jax import lax
from jax.experimental import pallas as pl
from jax.experimental.pallas import tpu as pltpu
from jax.sharding import Mesh
from jax.sharding import PartitionSpec as P

DK = 256
DV = 512
SPAN = 64
X, Z, C, Y = ("seq_0", "seq_1", "seq_2", "head")
SEQ = (X, Z, C)
F32 = jnp.float32
BF16 = jnp.bfloat16
MESH_ID = pl.DeviceIdType.MESH


def mm(a, b):
    return lax.dot_general(a, b, (((1,), (0,)), ((), ())), preferred_element_type=F32)


def mm_nt(a, b):
    return lax.dot_general(a, b, (((1,), (1,)), ((), ())), preferred_element_type=F32)


def mm_tn(a, b):
    return lax.dot_general(a, b, (((0,), (0,)), ((), ())), preferred_element_type=F32)


def remote(src, dst, send, recv, where):
    return pltpu.make_async_remote_copy(
        src_ref=src, dst_ref=dst, send_sem=send, recv_sem=recv,
        device_id=where, device_id_type=MESH_ID,
    )


def far_first(n):
    return sorted(range(1, n), key=lambda d: (-min(d, n - d), d))


def near_first(n):
    return sorted(range(1, n), key=lambda d: (min(d, n - d), d))


def body(
    nx, nz, tok, width,
    q_hbm, k_hbm, v_hbm, g_hbm, og_hbm, gain_hbm, w_hbm, out_hbm,
    q_v, k_v, v_v, g_v, og_v, gain_v, w_v,
    run_v, kd_v, qa_v, ka_v, b_v, c_v, d_v, q0_v, qp_v, wgt_v, wd_v, loc_v, gate_v,
    es_v, er_v, ss_v, sr_v, own_v,
    lzs_v, lz_v, zs_v, zr_v, pre_v, lxs_v, lx_v, xs_v, xr_v, zb_v, inc_v,
    ps_v, pr_v, k0_v, k1_v, p2s_v, p2r_v, o_v,
    in_sem, out_sem, e_sem, s_sem, lz_sem, z_sem, lx_sem, x_sem, b_sem, f_sem, p_sem, p2_sem,
):
    x, z, c, y = (lax.axis_index(n) for n in (X, Z, C, Y))
    half = DV // 2
    piece = half // nz
    y_a = y + 1 - 2 * (y % 2)
    y_b = 3 - y
    other = {C: 1 - c}

    barrier = pltpu.get_barrier_semaphore()
    peers = [other, {Y: y_a}, {Y: y_b}]
    peers += [{Z: (z + d) % nz} for d in range(1, nz)]
    peers += [{X: (x + d) % nx} for d in range(1, nx)]
    for peer in peers:
        pl.semaphore_signal(barrier, inc=1, device_id=peer, device_id_type=MESH_ID)

    loads = []
    for i, (src, dst) in enumerate((
        (g_hbm, g_v), (k_hbm, k_v), (v_hbm, v_v), (q_hbm, q_v),
        (og_hbm, og_v), (gain_hbm, gain_v), (w_hbm, w_v),
    )):
        copy = pltpu.make_async_copy(src, dst, in_sem.at[i])
        copy.start()
        loads.append(copy)
    load_g, load_k, load_v, load_q, load_og, load_gain, load_w = loads

    group = 256
    tri = (
        lax.broadcasted_iota(jnp.int32, (group, group), 0)
        >= lax.broadcasted_iota(jnp.int32, (group, group), 1)
    ).astype(BF16)
    load_g.wait()
    carry = jnp.zeros((1, DK), F32)
    for h in range(tok // group):
        rows = slice(h * group, (h + 1) * group)
        part = mm(tri, g_v[rows, :]) + carry
        run_v[rows, :] = part
        carry = part[group - 1:group, :]
    total = carry
    es_v[...] = jnp.broadcast_to(total, es_v.shape)

    pl.semaphore_wait(barrier, len(peers))
    e_copy = remote(es_v, er_v, e_sem.at[0], e_sem.at[1], other)
    e_copy.start()

    load_k.wait()

    def scale_keys(i, _):
        rows = pl.ds(pl.multiple_of(i * SPAN, SPAN), SPAN)
        kd_v[rows, :] = (k_v[rows, :].astype(F32) * jnp.exp(total - run_v[rows, :])).astype(BF16)
        return 0

    lax.fori_loop(0, tok // SPAN, scale_keys, 0)
    load_v.wait()
    there = pl.ds(pl.multiple_of((1 - c) * half, half), half)
    here = pl.ds(pl.multiple_of(c * half, half), half)
    ss_v[1 - c] = mm_tn(v_v[:, there], kd_v[...]).astype(BF16)
    s_copy = remote(ss_v.at[1 - c], sr_v.at[1 - c], s_sem.at[0], s_sem.at[1], other)
    s_copy.start()
    own_v[...] = mm_tn(v_v[:, here], kd_v[...])
    ss_v[c] = own_v[...].astype(BF16)
    s2_copy = remote(ss_v.at[c], sr_v.at[c], s_sem.at[2], s_sem.at[3], other)
    s2_copy.start()

    e_copy.wait_recv()
    partner = er_v[0:1, :]
    first = jnp.where(c == 0, total, partner)
    second = jnp.where(c == 0, partner, total)
    lzs_v[...] = jnp.broadcast_to(total + partner, lzs_v.shape)
    lz_v[z] = lzs_v[...]
    lz_copies = []
    for d in far_first(nz):
        copy = remote(lzs_v, lz_v.at[z], lz_sem.at[0, d], lz_sem.at[1, d], {Z: (z + d) % nz})
        copy.start()
        lz_copies.append(copy)

    s_copy.wait_recv()
    decay = jnp.exp(second)
    one = jnp.ones_like(decay)
    mine = jnp.where(c == 0, decay, one)
    theirs = jnp.where(c == 0, one, decay)

    for j in range(nz):
        rows = slice(j * piece, (j + 1) * piece)
        zs_v[j] = (own_v[rows, :] * mine + sr_v[c, rows, :].astype(F32) * theirs).astype(BF16)
    zr_v[z] = zs_v[z]
    z_copies = {}
    for d in far_first(nz):
        j = (z + d) % nz
        copy = remote(zs_v.at[j], zr_v.at[z], z_sem.at[0, d], z_sem.at[1, d], {Z: j})
        copy.start()
        z_copies[d] = copy

    load_q.wait()
    early = jnp.where(c == 0, jnp.zeros_like(first), first)

    def scale_pair(i, _):
        rows = pl.ds(pl.multiple_of(i * SPAN, SPAN), SPAN)
        r = run_v[rows, :]
        mid = run_v[pl.ds(pl.multiple_of(i * SPAN + SPAN // 2, 8), 1), :]
        q = q_v[rows, :].astype(F32)
        k = k_v[rows, :].astype(F32)
        qa_v[rows, :] = (q * jnp.exp(r - mid)).astype(BF16)
        ka_v[rows, :] = (k * jnp.exp(mid - r)).astype(BF16)
        q0_v[rows, :] = (q * jnp.exp(r)).astype(BF16)
        qp_v[rows, :] = (q * jnp.exp(r + early)).astype(BF16)
        return 0

    lax.fori_loop(0, tok // SPAN, scale_pair, 0)

    for copy in lz_copies:
        copy.wait_recv()
    slab = lz_v[0]
    for j in range(1, nz):
        slab = slab + lz_v[j]
    lxs_v[...] = slab
    lx_v[x] = slab
    lx_copies = []
    for d in range(1, nx):
        copy = remote(lxs_v, lx_v.at[x], lx_sem.at[0, d], lx_sem.at[1, d], {X: (x + d) % nx})
        copy.start()
        lx_copies.append(copy)

    for h, ref in ((SPAN, b_v), (2 * SPAN, c_v), (4 * SPAN, d_v)):
        for start in range(0, tok, 2 * h):
            edge = run_v[start + h - 1:start + h, :]

            def scale_cross(i, _, start=start, h=h, ref=ref, edge=edge):
                ke = pl.ds(pl.multiple_of(start + i * SPAN, SPAN), SPAN)
                qe = pl.ds(pl.multiple_of(start + h + i * SPAN, SPAN), SPAN)
                ref[ke, :] = (k_v[ke, :].astype(F32) * jnp.exp(edge - run_v[ke, :])).astype(BF16)
                ref[qe, :] = (q_v[qe, :].astype(F32) * jnp.exp(run_v[qe, :] - edge)).astype(BF16)
                return 0

            lax.fori_loop(0, h // SPAN, scale_cross, 0)

    for d in near_first(nz):
        z_copies[d].wait_recv()
    run = jnp.zeros((piece, DK), F32)
    for j in range(nz):
        pre_v[j] = run
        run = run * jnp.exp(lz_v[j, 0:1, :]) + zr_v[j].astype(F32)
    xs_v[...] = run.astype(BF16)
    xr_v[x] = xs_v[...]
    x_copies = []
    for d in far_first(nx):
        copy = remote(xs_v, xr_v.at[x], x_sem.at[0, d], x_sem.at[1, d], {X: (x + d) % nx})
        copy.start()
        x_copies.append(copy)

    wide = 2 * SPAN
    ti = lax.broadcasted_iota(jnp.int32, (wide, wide), 0)
    si = lax.broadcasted_iota(jnp.int32, (wide, wide), 1)
    same = (ti // SPAN) == (si // SPAN)
    causal = same & (ti >= si)
    across = (ti // SPAN) > (si // SPAN)
    for m in range(tok // wide):
        rows = slice(m * wide, (m + 1) * wide)
        inside = mm_nt(qa_v[rows, :], ka_v[rows, :])
        between = mm_nt(b_v[rows, :], b_v[rows, :])
        diag = jnp.where(causal, inside, jnp.where(across, between, 0.0)).astype(BF16)
        if m % 2 == 0:
            wgt_v[rows, 0:wide] = diag
            wgt_v[rows, wide:2 * wide] = jnp.zeros_like(diag)
        else:
            before = slice((m - 1) * wide, m * wide)
            wgt_v[rows, 0:wide] = mm_nt(c_v[rows, :], c_v[before, :]).astype(BF16)
            wgt_v[rows, wide:2 * wide] = diag
    wd_v[...] = mm_nt(d_v[group:2 * group, :], d_v[0:group, :]).astype(BF16)
    s2_copy.wait_recv()
    for h in range(2):
        rows = slice(h * group, (h + 1) * group)
        acc = mm(wgt_v[rows, :], v_v[rows, :])
        if h:
            acc = acc + mm(wd_v[...], v_v[0:group, :])
        loc_v[rows, :] = acc

    keep = jnp.where(c == 0, 0.0, 1.0).astype(F32)
    for e in range(2):
        cols = slice(e * half, (e + 1) * half)
        state = (sr_v[e].astype(F32) * keep).astype(BF16)
        for h in range(2):
            rows = slice(h * group, (h + 1) * group)
            loc_v[rows, cols] = loc_v[rows, cols] + mm_nt(q0_v[rows, :], state)

    for copy in lx_copies:
        copy.wait_recv()
    for copy in x_copies:
        copy.wait_recv()
    enter = jnp.zeros((piece, DK), F32)
    for j in range(nx):
        nxt = enter * jnp.exp(lx_v[j, 0:1, :]) + xr_v[j].astype(F32)
        enter = jnp.where(j < x, nxt, enter)
    log = jnp.zeros((1, DK), F32)
    for j in range(nz):
        zb_v[j] = (pre_v[j] + enter * jnp.exp(log)).astype(BF16)
        log = log + lz_v[j, 0:1, :]
    inc_v[c, z] = zb_v[z]
    b_copies = {}
    for d in far_first(nz):
        j = (z + d) % nz
        copy = remote(zb_v.at[j], inc_v.at[c, z], b_sem.at[0, d], b_sem.at[1, d], {Z: j})
        copy.start()
        b_copies[d] = copy
    f_copies = []
    copy = remote(inc_v.at[c, z], inc_v.at[c, z], f_sem.at[0, 0], f_sem.at[1, 0], other)
    copy.start()
    f_copies.append(copy)

    load_og.wait()
    load_gain.wait()

    def gate_rows(i, _):
        rows = pl.ds(pl.multiple_of(i * SPAN, SPAN), SPAN)
        u = og_v[rows, :].astype(F32)
        gate_v[rows, :] = gain_v[...] * (u / (1.0 + jnp.exp(-u)))
        return 0

    lax.fori_loop(0, tok // SPAN, gate_rows, 0)
    load_w.wait()

    for d in near_first(nz):
        b_copies[d].wait_recv()
        owner = (z + nz - d) % nz
        copy = remote(inc_v.at[c, owner], inc_v.at[c, owner], f_sem.at[0, d], f_sem.at[1, d], other)
        copy.start()
        f_copies.append(copy)
    for copy in f_copies:
        copy.wait_recv()

    def columns(block):
        return pl.ds(pl.multiple_of(block * width, width), width)

    chunks = tok // SPAN
    order = []
    for i in range(chunks // 2):
        order += [(i, 0), (i + chunks // 2, 1)]
    p_copies = {}
    for ch, side in order:
        rows = slice(ch * SPAN, (ch + 1) * SPAN)
        near, far = (y_a, y_b) if side == 0 else (y_b, y_a)
        att = loc_v[rows, :] + mm_nt(qp_v[rows, :], inc_v[...].reshape(DV, DK))
        spread = jnp.mean(att * att, axis=-1, keepdims=True)
        gated = (att * lax.rsqrt(spread + 1e-05) * gate_v[rows, :]).astype(BF16)
        theirs_far = 3 - near if side == 0 else near + 1 - 2 * (near % 2)
        ps_v[ch, 0] = mm(gated, w_v[:, columns(near)]).astype(BF16)
        ps_v[ch, 1] = mm(gated, w_v[:, columns(theirs_far)]).astype(BF16)
        copy = remote(ps_v.at[ch], pr_v.at[ch], p_sem.at[0, ch], p_sem.at[1, ch], {Y: near})
        copy.start()
        p_copies[ch] = copy
        k0_v[ch] = mm(gated, w_v[:, columns(y)])
        k1_v[ch] = mm(gated, w_v[:, columns(far)])
    p2_copies = {}
    for ch, side in order:
        far = y_b if side == 0 else y_a
        p_copies[ch].wait_recv()
        p2s_v[ch] = (k1_v[ch] + pr_v[ch, 1].astype(F32)).astype(BF16)
        copy = remote(p2s_v.at[ch], p2r_v.at[ch], p2_sem.at[0, ch], p2_sem.at[1, ch], {Y: far})
        copy.start()
        p2_copies[ch] = copy
        k0_v[ch] = k0_v[ch] + pr_v[ch, 0].astype(F32)
    outs = []
    for ch, side in order:
        p2_copies[ch].wait_recv()
        o_v[ch] = (k0_v[ch] + p2r_v[ch].astype(F32)).astype(BF16)
        copy = pltpu.make_async_copy(
            o_v.at[ch], out_hbm.at[pl.ds(ch * SPAN, SPAN), :], out_sem.at[ch]
        )
        copy.start()
        outs.append(copy)

    sent = [e_copy, s_copy, s2_copy] + lz_copies + list(z_copies.values()) + lx_copies
    sent += x_copies + list(b_copies.values()) + f_copies
    sent += list(p_copies.values()) + list(p2_copies.values())
    for copy in sent:
        copy.wait_send()
    for copy in outs:
        copy.wait()


def shards(nx, nz, queries, key_vectors, values, log_gate, out_gate, norm_gain, out_weight):
    tok = queries.shape[0]
    width = out_weight.shape[1] // 4
    piece = DV // 2 // nz
    chunks = tok // SPAN
    any_spec = pl.BlockSpec(memory_space=pl.ANY)
    vmem, dma = pltpu.VMEM, pltpu.SemaphoreType.DMA
    row = (tok, DK)
    scratch = [
        vmem(row, BF16), vmem(row, BF16), vmem((tok, DV), BF16), vmem(row, BF16),
        vmem((tok, DV), BF16), vmem((1, DV), F32), vmem(out_weight.shape, BF16),
        vmem(row, F32), vmem(row, BF16), vmem(row, BF16), vmem(row, BF16), vmem(row, BF16),
        vmem(row, BF16), vmem(row, BF16), vmem(row, BF16), vmem(row, BF16),
        vmem((tok, 256), BF16), vmem((256, 256), BF16), vmem((tok, DV), F32), vmem((tok, DV), F32),
        vmem((8, DK), F32), vmem((8, DK), F32),
        vmem((2, DV // 2, DK), BF16), vmem((2, DV // 2, DK), BF16), vmem((DV // 2, DK), F32),
        vmem((8, DK), F32), vmem((nz, 8, DK), F32),
        vmem((nz, piece, DK), BF16), vmem((nz, piece, DK), BF16), vmem((nz, piece, DK), F32),
        vmem((8, DK), F32), vmem((nx, 8, DK), F32),
        vmem((piece, DK), BF16), vmem((nx, piece, DK), BF16),
        vmem((nz, piece, DK), BF16), vmem((2, nz, piece, DK), BF16),
        vmem((chunks, 2, SPAN, width), BF16), vmem((chunks, 2, SPAN, width), BF16),
        vmem((chunks, SPAN, width), F32), vmem((chunks, SPAN, width), F32),
        vmem((chunks, SPAN, width), BF16), vmem((chunks, SPAN, width), BF16),
        vmem((chunks, SPAN, width), BF16),
        dma((7,)), dma((chunks,)), dma((2,)), dma((4,)), dma((2, nz)), dma((2, nz)),
        dma((2, nx)), dma((2, nx)), dma((2, nz)), dma((2, nz)), dma((2, chunks)), dma((2, chunks)),
    ]
    return pl.pallas_call(
        functools.partial(body, nx, nz, tok, width),
        out_shape=jax.ShapeDtypeStruct((tok, width), BF16),
        in_specs=[any_spec] * 7,
        out_specs=any_spec,
        scratch_shapes=scratch,
        compiler_params=pltpu.CompilerParams(
            collective_id=0, has_side_effects=True, vmem_limit_bytes=48 * 2**20
        ),
    )(queries, key_vectors, values, log_gate, out_gate, norm_gain.reshape(1, DV), out_weight)


def build(devices, nx, nz):
    split = Mesh(devices.reshape(nx, nz, 2, 4), (X, Z, C, Y))
    in_specs = (P(SEQ, Y),) * 5 + (P(Y), P(Y, None))
    return jax.shard_map(
        functools.partial(shards, nx, nz),
        mesh=split, in_specs=in_specs, out_specs=P(SEQ, Y), check_vma=False,
    )


def solution(mesh):
    return build(mesh.devices, 4, mesh.shape["seq"] // 8)
```

```python
import functools

import jax
import jax.numpy as jnp
from jax import lax
from jax.experimental import pallas as pl
from jax.experimental.pallas import tpu as pltpu
from jax.sharding import Mesh
from jax.sharding import PartitionSpec as P

DK = 256
DV = 512
SPAN = 64
X, Z, C, Y = ("seq_0", "seq_1", "seq_2", "head")
SEQ = (X, Z, C)
F32 = jnp.float32
BF16 = jnp.bfloat16
MESH_ID = pl.DeviceIdType.MESH
PROFILE = False


class Marks:
    def __init__(self):
        self.open = None

    def __call__(self, name):
        if not PROFILE:
            return
        if self.open is not None:
            self.open.__exit__(None, None, None)
        self.open = None
        if name:
            self.open = jax.named_scope(name)
            self.open.__enter__()


def mm(a, b):
    return lax.dot_general(a, b, (((1,), (0,)), ((), ())), preferred_element_type=F32)


def mm_nt(a, b):
    return lax.dot_general(a, b, (((1,), (1,)), ((), ())), preferred_element_type=F32)


def mm_tn(a, b):
    return lax.dot_general(a, b, (((0,), (0,)), ((), ())), preferred_element_type=F32)


def remote(src, dst, send, recv, where):
    return pltpu.make_async_remote_copy(
        src_ref=src, dst_ref=dst, send_sem=send, recv_sem=recv,
        device_id=where, device_id_type=MESH_ID,
    )


def far_first(n):
    return sorted(range(1, n), key=lambda d: (-min(d, n - d), d))


def near_first(n):
    return sorted(range(1, n), key=lambda d: (min(d, n - d), d))


def body(
    nx, nz, tok, width,
    q_hbm, k_hbm, v_hbm, g_hbm, og_hbm, gain_hbm, w_hbm, out_hbm,
    q_v, k_v, v_v, g_v, og_v, gain_v, w_v, wa_v, wb_v,
    run_v, kd_v, qa_v, ka_v, b_v, c_v, d_v, q0_v, qp_v, wgt_v, wd_v, loc_v, gate_v,
    es_v, er_v, ss_v, sr_v, own_v,
    lzs_v, lz_v, zs_v, zr_v, pre_v, lxs_v, lx_v, xs_v, xr_v, zb_v, inc_v,
    gs_v, gr_v, gm_v, rs_v, rr_v, k0_v, k1_v, fs_v, fr_v, o_v,
    in_sem, out_sem, e_sem, s_sem, lz_sem, z_sem, lx_sem, x_sem, b_sem, f_sem,
    wy_sem, wx_sem, wc_sem, wd_sem, g_sem, r_sem, n_sem,
):
    mark = Marks()
    x, z, c, y = (lax.axis_index(n) for n in (X, Z, C, Y))
    half = DV // 2
    piece = DV // nz
    y_a = y + 1 - 2 * (y % 2)
    y_b = 3 - y
    other = {C: 1 - c}
    z_to = [(z + d) % nz for d in range(nz)]
    z_from = [(z + nz - d) % nz for d in range(nz)]
    x_to = [(x + d) % nx for d in range(nx)]
    x_left = (x + nx - 1) % nx
    x_right = (x + 1) % nx

    e_copy = remote(es_v, er_v, e_sem.at[0], e_sem.at[1], other)
    s_copy = remote(ss_v, sr_v, s_sem.at[0], s_sem.at[1], other)
    lz_copies = {d: remote(lzs_v, lz_v.at[z], lz_sem.at[0, d], lz_sem.at[1, d], {Z: z_to[d]})
                 for d in range(1, nz)}
    z_copies = {d: remote(zs_v.at[z_to[d]], zr_v.at[z], z_sem.at[0, d], z_sem.at[1, d],
                          {Z: z_to[d]}) for d in range(1, nz)}
    lx_copies = {d: remote(lxs_v, lx_v.at[x], lx_sem.at[0, d], lx_sem.at[1, d], {X: x_to[d]})
                 for d in range(1, nx)}
    x_copies = {d: remote(xs_v, xr_v.at[x], x_sem.at[0, d], x_sem.at[1, d], {X: x_to[d]})
                for d in range(1, nx)}
    b_copies = {d: remote(zb_v.at[z_to[d]], inc_v.at[z], b_sem.at[0, d], b_sem.at[1, d],
                          {Z: z_to[d]}) for d in range(1, nz)}
    f_copies = {d: remote(inc_v.at[z_from[d]], inc_v.at[z_from[d]], f_sem.at[0, d],
                          f_sem.at[1, d], other) for d in range(nz)}

    parts = 8
    step = DV // 2 // parts

    def w_rows(parity, k):
        return pl.ds(pl.multiple_of(parity * (DV // 2) + k * step, step), step)

    near_half, far_half = x % 2, 1 - x % 2

    def wy(s, k):
        rows = w_rows(near_half, k)
        dst, to = ((wa_v, y_a), (wb_v, y_b))[s]
        return remote(w_v.at[rows, :], dst.at[rows, :], wy_sem.at[0, s, k], wy_sem.at[1, s, k],
                      {Y: to})

    def wx(s, k):
        rows = w_rows(near_half, k)
        buf, to = ((wa_v, x_left), (wb_v, x_right))[s]
        return remote(buf.at[rows, :], buf.at[rows, :], wx_sem.at[0, s, k], wx_sem.at[1, s, k],
                      {X: to})

    def wc(s, k):
        rows = w_rows(near_half, k)
        buf = (wa_v, wb_v)[s]
        return remote(buf.at[rows, :], buf.at[rows, :], wc_sem.at[0, s, k], wc_sem.at[1, s, k],
                      other)

    def wd(s, k):
        rows = w_rows(far_half, k)
        buf = (wa_v, wb_v)[s]
        return remote(buf.at[rows, :], buf.at[rows, :], wd_sem.at[0, s, k], wd_sem.at[1, s, k],
                      other)

    def pass_near(k):
        for s in range(2):
            wy(s, k).wait_recv()
            wx(s, k).start()
            wc(s, k).start()

    def pass_far(k):
        for s in range(2):
            wx(s, k).wait_recv()
            wd(s, k).start()

    def repeat(low, high, f):
        def one(k, _):
            f(k)
            return 0

        lax.fori_loop(low, high, one, 0)

    barrier = pltpu.get_barrier_semaphore()

    def greet(peers):
        for peer in peers:
            pl.semaphore_signal(barrier, inc=1, device_id=peer, device_id_type=MESH_ID)

    greet([other, {Y: y_a}, {Y: y_b}])

    @pl.when(c == 0)
    def _():
        greet([{X: x_left}, {X: x_right}])

    @pl.when(c == 1)
    def _():
        greet([{Z: z_to[d]} for d in range(1, nz)] + [{X: x_to[d]} for d in range(1, nx)])

    loads = []
    for i, (src, dst) in enumerate((
        (g_hbm, g_v), (k_hbm, k_v), (v_hbm, v_v), (w_hbm, w_v), (q_hbm, q_v),
        (og_hbm, og_v), (gain_hbm, gain_v),
    )):
        copy = pltpu.make_async_copy(src, dst, in_sem.at[i])
        copy.start()
        loads.append(copy)
    load_g, load_k, load_v, load_w, load_q, load_og, load_gain = loads

    group = 256
    tri = (
        lax.broadcasted_iota(jnp.int32, (group, group), 0)
        >= lax.broadcasted_iota(jnp.int32, (group, group), 1)
    ).astype(BF16)
    mark("w_g")
    load_g.wait()
    mark("cumsum")
    carry = jnp.zeros((1, DK), F32)
    for h in range(tok // group):
        rows = slice(h * group, (h + 1) * group)
        part = mm(tri, g_v[rows, :]) + carry
        run_v[rows, :] = part
        carry = part[group - 1:group, :]
    total = carry
    es_v[...] = total

    mark("keys")
    load_k.wait()

    def scale_keys(i):
        rows = pl.ds(pl.multiple_of(i * SPAN, SPAN), SPAN)
        kd_v[rows, :] = (k_v[rows, :].astype(F32) * jnp.exp(total - run_v[rows, :])).astype(BF16)

    repeat(0, tok // SPAN, scale_keys)
    mark("state")
    load_v.wait()
    for e in range(2):
        rows = slice(e * half, (e + 1) * half)
        own_v[rows, :] = mm_tn(v_v[:, rows], kd_v[...])
        ss_v[rows, :] = own_v[rows, :].astype(BF16)

    mark("w_barrier")

    @pl.when(c == 0)
    def _():
        pl.semaphore_wait(barrier, 5)
        e_copy.start()
        s_copy.start()
        load_w.wait()
        for k in range(parts):
            for s in range(2):
                wy(s, k).start()
        er_v[...] = jnp.zeros_like(er_v)

    @pl.when(c == 1)
    def _():
        pl.semaphore_wait(barrier, 3 + nz - 1 + nx - 1)

    mark("w_e")

    @pl.when(c == 1)
    def _():
        e_copy.wait_recv()
        lzs_v[...] = total + er_v[...]
        lz_v[z] = lzs_v[...]
        for d in far_first(nz):
            lz_copies[d].start()

    early = er_v[...]
    mark("w_s")

    @pl.when(c == 1)
    def _():
        s_copy.wait_recv()

    mark("chip_state")

    @pl.when(c == 1)
    def _():
        decay = jnp.exp(total)
        for j in range(nz):
            rows = slice(j * piece, (j + 1) * piece)
            zs_v[j] = (own_v[rows, :] + sr_v[rows, :].astype(F32) * decay).astype(BF16)
        for d in far_first(nz):
            z_copies[d].start()
        zr_v[z] = zs_v[z]
        load_w.wait()

    mark("scale_pair")
    load_q.wait()

    def scale_pair(i):
        rows = pl.ds(pl.multiple_of(i * SPAN, SPAN), SPAN)
        r = run_v[rows, :]
        mid = run_v[pl.ds(pl.multiple_of(i * SPAN + SPAN // 2, 8), 1), :]
        q = q_v[rows, :].astype(F32)
        k = k_v[rows, :].astype(F32)
        qa_v[rows, :] = (q * jnp.exp(r - mid)).astype(BF16)
        ka_v[rows, :] = (k * jnp.exp(mid - r)).astype(BF16)
        q0_v[rows, :] = (q * jnp.exp(r)).astype(BF16)
        qp_v[rows, :] = (q * jnp.exp(r + early)).astype(BF16)

    repeat(0, tok // SPAN, scale_pair)

    mark("scale_cross")
    for h, ref in ((SPAN, b_v), (2 * SPAN, c_v), (4 * SPAN, d_v)):
        for start in range(0, tok, 2 * h):
            edge = run_v[start + h - 1:start + h, :]

            def scale_cross(i, start=start, h=h, ref=ref, edge=edge):
                ke = pl.ds(pl.multiple_of(start + i * SPAN, SPAN), SPAN)
                qe = pl.ds(pl.multiple_of(start + h + i * SPAN, SPAN), SPAN)
                ref[ke, :] = (k_v[ke, :].astype(F32) * jnp.exp(edge - run_v[ke, :])).astype(BF16)
                ref[qe, :] = (q_v[qe, :].astype(F32) * jnp.exp(run_v[qe, :] - edge)).astype(BF16)

            repeat(0, h // SPAN, scale_cross)

    mark("attn")
    wide = 2 * SPAN
    ti = lax.broadcasted_iota(jnp.int32, (wide, wide), 0)
    si = lax.broadcasted_iota(jnp.int32, (wide, wide), 1)
    same = (ti // SPAN) == (si // SPAN)
    causal = same & (ti >= si)
    across = (ti // SPAN) > (si // SPAN)
    for m in range(tok // wide):
        rows = slice(m * wide, (m + 1) * wide)
        inside = mm_nt(qa_v[rows, :], ka_v[rows, :])
        between = mm_nt(b_v[rows, :], b_v[rows, :])
        diag = jnp.where(causal, inside, jnp.where(across, between, 0.0)).astype(BF16)
        if m % 2 == 0:
            wgt_v[rows, 0:wide] = diag
            wgt_v[rows, wide:2 * wide] = jnp.zeros_like(diag)
        else:
            before = slice((m - 1) * wide, m * wide)
            wgt_v[rows, 0:wide] = mm_nt(c_v[rows, :], c_v[before, :]).astype(BF16)
            wgt_v[rows, wide:2 * wide] = diag
    wd_v[...] = mm_nt(d_v[group:2 * group, :], d_v[0:group, :]).astype(BF16)
    for h in range(2):
        rows = slice(h * group, (h + 1) * group)
        acc = mm(wgt_v[rows, :], v_v[rows, :])
        if h:
            acc = acc + mm(wd_v[...], v_v[0:group, :])
        loc_v[rows, :] = acc

    @pl.when(c == 1)
    def _():
        for h in range(2):
            rows = slice(h * group, (h + 1) * group)
            loc_v[rows, :] = loc_v[rows, :] + mm_nt(q0_v[rows, :], sr_v[...])

    mark("gate")
    load_og.wait()
    load_gain.wait()

    def gate_rows(i):
        rows = pl.ds(pl.multiple_of(i * SPAN, SPAN), SPAN)
        u = og_v[rows, :].astype(F32)
        gate_v[rows, :] = gain_v[...] * (u / (1.0 + jnp.exp(-u)))

    repeat(0, tok // SPAN, gate_rows)

    mark("w_lz")

    @pl.when(c == 1)
    def _():
        for d in near_first(nz):
            lz_copies[d].wait_recv()
        slab = lz_v[0]
        for j in range(1, nz):
            slab = slab + lz_v[j]
        lxs_v[...] = slab
        lx_v[x] = slab
        for d in range(1, nx):
            lx_copies[d].start()

    mark("w_z")

    @pl.when(c == 1)
    def _():
        for d in near_first(nz):
            z_copies[d].wait_recv()

    mark("zprefix")

    @pl.when(c == 1)
    def _():
        run = jnp.zeros((piece, DK), F32)
        for j in range(nz):
            pre_v[j] = run
            run = run * jnp.exp(lz_v[j]) + zr_v[j].astype(F32)
        xs_v[...] = run.astype(BF16)
        for d in far_first(nx):
            x_copies[d].start()
        xr_v[x] = xs_v[...]

    mark("w_x")

    @pl.when(c == 1)
    def _():
        for d in range(1, nx):
            lx_copies[d].wait_recv()
        for d in near_first(nx):
            x_copies[d].wait_recv()

    mark("xprefix")

    @pl.when(c == 1)
    def _():
        enter = jnp.zeros((piece, DK), F32)
        for j in range(nx):
            nxt = enter * jnp.exp(lx_v[j]) + xr_v[j].astype(F32)
            enter = jnp.where(j < x, nxt, enter)
        log = jnp.zeros((1, DK), F32)
        for j in range(nz):
            zb_v[j] = (pre_v[j] + enter * jnp.exp(log)).astype(BF16)
            log = log + lz_v[j]
        for d in far_first(nz):
            b_copies[d].start()
        inc_v[z] = zb_v[z]
        f_copies[0].start()

    mark("w_b")

    @pl.when(c == 1)
    def _():
        for d in near_first(nz):
            b_copies[d].wait_recv()
            f_copies[d].start()

    mark("weights")
    ahead = 3

    @pl.when(c == 0)
    def _():
        def both(k):
            pass_near(k)
            pass_far(k - ahead)

        repeat(0, ahead, pass_near)
        repeat(ahead, parts, both)

    mark("w_f")

    @pl.when(c == 0)
    def _():
        for d in range(nz):
            f_copies[d].wait_recv()

    mark("gated")

    def columns(block):
        return pl.ds(pl.multiple_of(block * width, width), width)

    sides = (
        (y_a, y_b, y_b + 1 - 2 * (y_b % 2), ((y + 1) // 2) % 2, wa_v),
        (y_b, y_a, 3 - y_a, y // 2, wb_v),
    )
    side_tok = tok // 2
    chunks = side_tok // 2 // SPAN

    def start_row(s, own, j):
        lead = sides[s][3] if own else 1 - sides[s][3]
        return pl.multiple_of(s * side_tok + lead * (side_tok // 2) + j * SPAN, SPAN)

    def gated_rows(s, own, j):
        rows = pl.ds(start_row(s, own, j), SPAN)
        att = loc_v[rows, :] + mm_nt(qp_v[rows, :], inc_v[...].reshape(DV, DK))
        spread = jnp.mean(att * att, axis=-1, keepdims=True)
        return (att * lax.rsqrt(spread + 1e-05) * gate_v[rows, :]).astype(BF16)

    order = [(s, j) for j in range(chunks) for s in range(2)]
    g_copies, r_copies, n_copies = {}, {}, {}
    for s, j in order:
        gs_v[s, j] = gated_rows(s, False, j)
        g_copies[s, j] = remote(gs_v.at[s, j], gr_v.at[s, j], g_sem.at[0, s, j],
                                g_sem.at[1, s, j], {Y: sides[s][0]})
        g_copies[s, j].start()
    for s, j in order:
        gm_v[s, j] = gated_rows(s, True, j)

    mark("w_weights")

    @pl.when(c == 0)
    def _():
        repeat(parts - ahead, parts, pass_far)

    @pl.when(c == 1)
    def _():
        def arrive(k):
            for s in range(2):
                wc(s, k).wait_recv()
                wd(s, k).wait_recv()

        repeat(0, parts, arrive)

    mark("proj")

    def pair_sum(s, j, block):
        cols = columns(block)
        return mm(gm_v[s, j], w_v[:, cols]) + mm(gr_v[s, j], sides[s][4][:, cols])

    for s, j in order:
        near, far, far_near = sides[s][:3]
        g_copies[s, j].wait_recv()
        rs_v[s, j, 0] = pair_sum(s, j, far).astype(BF16)
        rs_v[s, j, 1] = pair_sum(s, j, far_near).astype(BF16)
        r_copies[s, j] = remote(rs_v.at[s, j], rr_v.at[s, j], r_sem.at[0, s, j],
                                r_sem.at[1, s, j], {Y: far})
        r_copies[s, j].start()
    mark("keep")
    for s, j in order:
        k1_v[s, j] = pair_sum(s, j, sides[s][0])
        k0_v[s, j] = pair_sum(s, j, y)
    mark("sum")
    outs = []

    def put(src, row, i):
        copy = pltpu.make_async_copy(src, out_hbm.at[pl.ds(row, SPAN), :], out_sem.at[i])
        copy.start()
        outs.append(copy)

    for s, j in order:
        r_copies[s, j].wait_recv()
        fs_v[s, j] = (k1_v[s, j] + rr_v[s, j, 1].astype(F32)).astype(BF16)
        n_copies[s, j] = remote(fs_v.at[s, j], fr_v.at[s, j], n_sem.at[0, s, j],
                                n_sem.at[1, s, j], {Y: sides[s][0]})
        n_copies[s, j].start()
        o_v[s, j] = (k0_v[s, j] + rr_v[s, j, 0].astype(F32)).astype(BF16)
        put(o_v.at[s, j], start_row(s, True, j), len(outs))
    mark("last")
    for s, j in order:
        n_copies[s, j].wait_recv()
        put(fr_v.at[s, j], start_row(s, False, j), len(outs))

    mark("drain")

    @pl.when(c == 0)
    def _():
        e_copy.wait_send()
        s_copy.wait_send()

        def sent(k):
            for s in range(2):
                for copy in (wy, wx, wc, wd):
                    copy(s, k).wait_send()

        repeat(0, parts, sent)

    @pl.when(c == 1)
    def _():
        for group_of in (lz_copies, z_copies, lx_copies, x_copies, b_copies, f_copies):
            for copy in group_of.values():
                copy.wait_send()

    for group_of in (g_copies, r_copies, n_copies):
        for copy in group_of.values():
            copy.wait_send()
    for copy in outs:
        copy.wait()
    mark(None)


def shards(nx, nz, queries, key_vectors, values, log_gate, out_gate, norm_gain, out_weight):
    tok = queries.shape[0]
    width = out_weight.shape[1] // 4
    piece = DV // nz
    chunks = tok // 4 // SPAN
    any_spec = pl.BlockSpec(memory_space=pl.ANY)
    vmem, dma = pltpu.VMEM, pltpu.SemaphoreType.DMA
    row = (tok, DK)
    weights = vmem(out_weight.shape, BF16)
    blocks = (2, chunks, SPAN, width)
    scratch = [
        vmem(row, BF16), vmem(row, BF16), vmem((tok, DV), BF16), vmem(row, BF16),
        vmem((tok, DV), BF16), vmem((1, DV), F32), weights, weights, weights,
        vmem(row, F32), vmem(row, BF16), vmem(row, BF16), vmem(row, BF16), vmem(row, BF16),
        vmem(row, BF16), vmem(row, BF16), vmem(row, BF16), vmem(row, BF16),
        vmem((tok, 256), BF16), vmem((256, 256), BF16), vmem((tok, DV), F32), vmem((tok, DV), F32),
        vmem((1, DK), F32), vmem((1, DK), F32),
        vmem((DV, DK), BF16), vmem((DV, DK), BF16), vmem((DV, DK), F32),
        vmem((1, DK), F32), vmem((nz, 1, DK), F32),
        vmem((nz, piece, DK), BF16), vmem((nz, piece, DK), BF16), vmem((nz, piece, DK), F32),
        vmem((1, DK), F32), vmem((nx, 1, DK), F32),
        vmem((piece, DK), BF16), vmem((nx, piece, DK), BF16),
        vmem((nz, piece, DK), BF16), vmem((nz, piece, DK), BF16),
        vmem(blocks, BF16), vmem(blocks, BF16), vmem(blocks, BF16),
        vmem((2, chunks, 2, SPAN, width), BF16), vmem((2, chunks, 2, SPAN, width), BF16),
        vmem(blocks, F32), vmem(blocks, F32),
        vmem(blocks, BF16), vmem(blocks, BF16), vmem(blocks, BF16),
        dma((7,)), dma((4 * chunks,)), dma((2,)), dma((2,)), dma((2, nz)), dma((2, nz)),
        dma((2, nx)), dma((2, nx)), dma((2, nz)), dma((2, nz)),
        dma((2, 2, 8)), dma((2, 2, 8)), dma((2, 2, 8)), dma((2, 2, 8)),
        dma((2, 2, chunks)), dma((2, 2, chunks)), dma((2, 2, chunks)),
    ]
    return pl.pallas_call(
        functools.partial(body, nx, nz, tok, width),
        out_shape=jax.ShapeDtypeStruct((tok, width), BF16),
        in_specs=[any_spec] * 7,
        out_specs=any_spec,
        scratch_shapes=scratch,
        compiler_params=pltpu.CompilerParams(
            collective_id=0, has_side_effects=True, vmem_limit_bytes=67043328
        ),
    )(queries, key_vectors, values, log_gate, out_gate, norm_gain.reshape(1, DV), out_weight)


def build(devices, nx, nz):
    split = Mesh(devices.reshape(nx, nz, 2, 4), (X, Z, C, Y))
    in_specs = (P(SEQ, Y),) * 5 + (P(Y), P(Y, None))
    return jax.shard_map(
        functools.partial(shards, nx, nz),
        mesh=split, in_specs=in_specs, out_specs=P(SEQ, Y), check_vma=False,
    )


def solution(mesh):
    return build(mesh.devices, 4, mesh.shape["seq"] // 8)
```

```python
import functools

import jax
import jax.numpy as jnp
from jax import lax
from jax.experimental import pallas as pl
from jax.experimental.pallas import tpu as pltpu
from jax.sharding import Mesh
from jax.sharding import PartitionSpec as P

DK = 256
DV = 512
SPAN = 64
X, Z, C, Y = ("seq_0", "seq_1", "seq_2", "head")
SEQ = (X, Z, C)
F32 = jnp.float32
BF16 = jnp.bfloat16
MESH_ID = pl.DeviceIdType.MESH
PROFILE = False


class Marks:
    def __init__(self):
        self.open = None

    def __call__(self, name):
        if not PROFILE:
            return
        if self.open is not None:
            self.open.__exit__(None, None, None)
        self.open = None
        if name:
            self.open = jax.named_scope(name)
            self.open.__enter__()


def mm(a, b):
    return lax.dot_general(a, b, (((1,), (0,)), ((), ())), preferred_element_type=F32)


def mm_nt(a, b):
    return lax.dot_general(a, b, (((1,), (1,)), ((), ())), preferred_element_type=F32)


def mm_tn(a, b):
    return lax.dot_general(a, b, (((0,), (0,)), ((), ())), preferred_element_type=F32)


def remote(src, dst, send, recv, where):
    return pltpu.make_async_remote_copy(
        src_ref=src, dst_ref=dst, send_sem=send, recv_sem=recv,
        device_id=where, device_id_type=MESH_ID,
    )


def far_first(n):
    return sorted(range(1, n), key=lambda d: (-min(d, n - d), d))


def near_first(n):
    return sorted(range(1, n), key=lambda d: (min(d, n - d), d))


def body(
    nx, nz, tok, width,
    q_hbm, k_hbm, v_hbm, g_hbm, og_hbm, gain_hbm, w_hbm, out_hbm,
    q_v, k_v, v_v, g_v, og_v, gain_v, w_v, wn_v,
    run_v, kd_v, qa_v, ka_v, b_v, c_v, d_v, q0_v, qp_v, wgt_v, wd_v, loc_v, gate_v,
    es_v, er_v, ss_v, sr_v, own_v,
    lzs_v, lz_v, zs_v, zr_v, pre_v, lxs_v, lx_v, xs_v, xr_v, ent_v, zb_v, inc_v,
    gs_v, gr_v, gm_v, rs_v, rr_v, k0_v, k1_v, fs_v, fr_v, o_v,
    in_sem, out_sem, e_sem, s_sem, lz_sem, z_sem, lx_sem, x_sem, b_sem, f_sem,
    wy_sem, wx_sem, wc_sem, g_sem, r_sem, n_sem,
):
    mark = Marks()
    x, z, c, y = (lax.axis_index(n) for n in (X, Z, C, Y))
    half = DV // 2
    piece = DV // nz
    y_a = y + 1 - 2 * (y % 2)
    y_b = 3 - y
    other = {C: 1 - c}
    z_to = [(z + d) % nz for d in range(nz)]
    z_from = [(z + nz - d) % nz for d in range(nz)]
    x_to = [(x + d) % nx for d in range(nx)]
    x_left = (x + nx - 1) % nx
    x_right = (x + 1) % nx

    e_copy = remote(es_v, er_v, e_sem.at[0], e_sem.at[1], other)
    s_copy = remote(ss_v, sr_v, s_sem.at[0], s_sem.at[1], other)
    most = pl.ds(0, nz - 1)
    lz_copies = {d: remote(lzs_v, lz_v.at[z], lz_sem.at[0], lz_sem.at[1], {Z: z_to[d]})
                 for d in range(1, nz)}
    lz_all = remote(lz_v.at[most], lz_v.at[most], lz_sem.at[0], lz_sem.at[1], other)
    z_copies = {d: remote(zs_v.at[z_to[d]], zr_v.at[z], z_sem.at[0], z_sem.at[1],
                          {Z: z_to[d]}) for d in range(1, nz)}
    z_all = remote(zs_v.at[most], zr_v.at[most], z_sem.at[0], z_sem.at[1], other)
    lx_copies = {d: remote(lxs_v, lx_v.at[x], lx_sem.at[0, d - 1], lx_sem.at[1, d - 1],
                           {X: x_to[d]}) for d in range(1, nx)}
    x_copies = {d: remote(xs_v, xr_v.at[x], x_sem.at[0, d - 1], x_sem.at[1, d - 1],
                          {X: x_to[d]}) for d in range(1, nx)}
    b_copies = {d: remote(zb_v.at[z_to[d]], inc_v.at[z], b_sem.at[0], b_sem.at[d],
                          {Z: z_to[d]}) for d in range(1, nz)}
    b_all = remote(zb_v.at[most], inc_v.at[most], b_sem.at[0], b_sem.at[1], other)
    f_copies = {d: remote(inc_v.at[z_from[d]], inc_v.at[z_from[d]], f_sem.at[0],
                          f_sem.at[1], other) for d in range(nz)}
    f_all = remote(inc_v, inc_v, f_sem.at[0], f_sem.at[1], other)

    def step_a(v):
        return v + 1 - 2 * (v % 2)

    def near_of(s, v):
        return jnp.where(s == 0, step_a(v), 3 - v)

    def far_of(s, v):
        return jnp.where(s == 0, 3 - v, step_a(v))

    def columns(block):
        return pl.ds(pl.multiple_of(block * width, width), width)

    parts = 4
    step = DV // 2

    def w_part(s, owner, parity, k):
        far = far_of(s, owner)
        block = (far, near_of(s, far), near_of(s, owner), owner)[k]
        return pl.ds(pl.multiple_of(parity * step, step), step), columns(block)

    near_half, far_half = x % 2, 1 - x % 2

    def wy(s, k):
        to = near_of(s, y)
        rows, cols = w_part(s, to, near_half, k)
        return remote(w_v.at[rows, cols], wn_v.at[s, rows, cols], wy_sem.at[0], wy_sem.at[1 + k],
                      {Y: to})

    def passed(s, k, parity, send, recv, to):
        rows, cols = w_part(s, y, parity, k)
        buf = wn_v.at[s, rows, cols]
        return remote(buf, buf, send, recv, to)

    def wx(s, k):
        return passed(s, k, near_half, wx_sem.at[0], wx_sem.at[1 + k], {X: (x_left, x_right)[s]})

    def wc(s, k):
        return passed(s, k, near_half, wc_sem.at[0], wc_sem.at[1 + k // 2], other)

    def wd(s, k):
        return passed(s, k, far_half, wc_sem.at[0], wc_sem.at[1 + k // 2], other)

    def part_wait(sem, k):
        two = wn_v.at[:, pl.ds(0, step), pl.ds(0, width)]
        remote(two, two, sem.at[0], sem.at[1 + k], other).wait_recv()

    def pass_near(k):
        part_wait(wy_sem, k)
        for s in range(2):
            wx(s, k).start()
            wc(s, k).start()

    def pass_far(k):
        part_wait(wx_sem, k)
        for s in range(2):
            wd(s, k).start()

    def repeat(low, high, f):
        def one(k, _):
            f(k)
            return 0

        lax.fori_loop(low, high, one, 0)

    barrier = pltpu.get_barrier_semaphore()

    def greet(peers):
        for peer in peers:
            pl.semaphore_signal(barrier, inc=1, device_id=peer, device_id_type=MESH_ID)

    greet([other, {Y: y_a}, {Y: y_b}])

    @pl.when(c == 0)
    def _():
        greet([{X: x_left}, {X: x_right}])

    @pl.when(c == 1)
    def _():
        greet([{Z: z_to[d]} for d in range(1, nz)] + [{X: x_to[d]} for d in range(1, nx)])

    loads = []
    for i, (src, dst) in enumerate((
        (g_hbm, g_v), (k_hbm, k_v), (v_hbm, v_v), (w_hbm, w_v), (q_hbm, q_v),
        (og_hbm, og_v), (gain_hbm, gain_v),
    )):
        copy = pltpu.make_async_copy(src, dst, in_sem.at[i])
        copy.start()
        loads.append(copy)
    load_g, load_k, load_v, load_w, load_q, load_og, load_gain = loads

    group = 256
    tri = (
        lax.broadcasted_iota(jnp.int32, (group, group), 0)
        >= lax.broadcasted_iota(jnp.int32, (group, group), 1)
    ).astype(BF16)
    mark("w_g")
    load_g.wait()
    mark("cumsum")
    carry = jnp.zeros((1, DK), F32)
    for h in range(tok // group):
        rows = slice(h * group, (h + 1) * group)
        part = mm(tri, g_v[rows, :]) + carry
        run_v[rows, :] = part
        carry = part[group - 1:group, :]
    total = carry
    es_v[...] = total

    mark("keys")
    load_k.wait()

    def scale_keys(i):
        rows = pl.ds(pl.multiple_of(i * SPAN, SPAN), SPAN)
        kd_v[rows, :] = (k_v[rows, :].astype(F32) * jnp.exp(total - run_v[rows, :])).astype(BF16)

    repeat(0, tok // SPAN, scale_keys)
    mark("state")
    load_v.wait()
    for e in range(2):
        rows = slice(e * half, (e + 1) * half)
        own_v[rows, :] = mm_tn(v_v[:, rows], kd_v[...])
        ss_v[rows, :] = own_v[rows, :].astype(BF16)

    mark("w_barrier")

    @pl.when(c == 0)
    def _():
        pl.semaphore_wait(barrier, 5)
        e_copy.start()
        s_copy.start()
        load_w.wait()
        for k in range(parts):
            for s in range(2):
                wy(s, k).start()
        er_v[...] = jnp.zeros_like(er_v)

    @pl.when(c == 1)
    def _():
        pl.semaphore_wait(barrier, 3 + nz - 1 + nx - 1)

    mark("w_e")

    @pl.when(c == 1)
    def _():
        e_copy.wait_recv()
        lzs_v[...] = total + er_v[...]
        lz_v[z] = lzs_v[...]
        for d in far_first(nz):
            lz_copies[d].start()

    early = er_v[...]
    mark("w_s")

    @pl.when(c == 1)
    def _():
        s_copy.wait_recv()

    mark("chip_state")

    @pl.when(c == 1)
    def _():
        decay = jnp.exp(total)
        for j in range(nz):
            rows = slice(j * piece, (j + 1) * piece)
            zs_v[j] = (own_v[rows, :] + sr_v[rows, :].astype(F32) * decay).astype(BF16)
        for d in far_first(nz):
            z_copies[d].start()
        zr_v[z] = zs_v[z]
        load_w.wait()

    mark("scale_pair")
    load_q.wait()

    def scale_pair(i):
        rows = pl.ds(pl.multiple_of(i * SPAN, SPAN), SPAN)
        r = run_v[rows, :]
        mid = run_v[pl.ds(pl.multiple_of(i * SPAN + SPAN // 2, 8), 1), :]
        q = q_v[rows, :].astype(F32)
        k = k_v[rows, :].astype(F32)
        qa_v[rows, :] = (q * jnp.exp(r - mid)).astype(BF16)
        ka_v[rows, :] = (k * jnp.exp(mid - r)).astype(BF16)
        q0_v[rows, :] = (q * jnp.exp(r)).astype(BF16)
        qp_v[rows, :] = (q * jnp.exp(r + early)).astype(BF16)

    repeat(0, tok // SPAN, scale_pair)

    mark("scale_cross")
    for h, ref in ((SPAN, b_v), (2 * SPAN, c_v), (4 * SPAN, d_v)):
        for start in range(0, tok, 2 * h):
            edge = run_v[start + h - 1:start + h, :]

            def scale_cross(i, start=start, h=h, ref=ref, edge=edge):
                ke = pl.ds(pl.multiple_of(start + i * SPAN, SPAN), SPAN)
                qe = pl.ds(pl.multiple_of(start + h + i * SPAN, SPAN), SPAN)
                ref[ke, :] = (k_v[ke, :].astype(F32) * jnp.exp(edge - run_v[ke, :])).astype(BF16)
                ref[qe, :] = (q_v[qe, :].astype(F32) * jnp.exp(run_v[qe, :] - edge)).astype(BF16)

            repeat(0, h // SPAN, scale_cross)

    mark("attn")
    wide = 2 * SPAN
    ti = lax.broadcasted_iota(jnp.int32, (wide, wide), 0)
    si = lax.broadcasted_iota(jnp.int32, (wide, wide), 1)
    same = (ti // SPAN) == (si // SPAN)
    causal = same & (ti >= si)
    across = (ti // SPAN) > (si // SPAN)
    for m in range(tok // wide):
        rows = slice(m * wide, (m + 1) * wide)
        inside = mm_nt(qa_v[rows, :], ka_v[rows, :])
        between = mm_nt(b_v[rows, :], b_v[rows, :])
        diag = jnp.where(causal, inside, jnp.where(across, between, 0.0)).astype(BF16)
        if m % 2 == 0:
            wgt_v[rows, 0:wide] = diag
            wgt_v[rows, wide:2 * wide] = jnp.zeros_like(diag)
        else:
            before = slice((m - 1) * wide, m * wide)
            wgt_v[rows, 0:wide] = mm_nt(c_v[rows, :], c_v[before, :]).astype(BF16)
            wgt_v[rows, wide:2 * wide] = diag
    wd_v[...] = mm_nt(d_v[group:2 * group, :], d_v[0:group, :]).astype(BF16)
    for h in range(2):
        rows = slice(h * group, (h + 1) * group)
        acc = mm(wgt_v[rows, :], v_v[rows, :])
        if h:
            acc = acc + mm(wd_v[...], v_v[0:group, :])
        loc_v[rows, :] = acc

    @pl.when(c == 1)
    def _():
        for h in range(2):
            rows = slice(h * group, (h + 1) * group)
            loc_v[rows, :] = loc_v[rows, :] + mm_nt(q0_v[rows, :], sr_v[...])

    mark("gate")
    load_og.wait()
    load_gain.wait()

    def gate_rows(i):
        rows = pl.ds(pl.multiple_of(i * SPAN, SPAN), SPAN)
        u = og_v[rows, :].astype(F32)
        gate_v[rows, :] = gain_v[...] * (u / (1.0 + jnp.exp(-u)))

    repeat(0, tok // SPAN, gate_rows)

    mark("w_lz")

    @pl.when(c == 1)
    def _():
        lz_all.wait_recv()
        slab = lz_v[0]
        for j in range(1, nz):
            slab = slab + lz_v[j]
        lxs_v[...] = slab
        for d in range(1, nx):
            pl.when(x + d < nx)(lx_copies[d].start)

    mark("w_z")

    @pl.when(c == 1)
    def _():
        z_all.wait_recv()

    mark("zprefix")

    @pl.when(c == 1)
    def _():
        run = jnp.zeros((piece, DK), F32)
        for j in range(nz):
            pre_v[j] = run
            run = run * jnp.exp(lz_v[j]) + zr_v[j].astype(F32)
        xs_v[...] = run.astype(BF16)
        for d in far_first(nx):
            pl.when(x + d < nx)(x_copies[d].start)

    mark("w_x")

    @pl.when(c == 1)
    def _():
        for d in range(1, nx):
            pl.when(x >= d)(lx_copies[d].wait_recv)
        for d in near_first(nx):
            pl.when(x >= d)(x_copies[d].wait_recv)

    mark("xprefix")

    @pl.when(c == 1)
    def _():
        ent_v[...] = jnp.zeros_like(ent_v)
        for j in range(nx - 1):
            @pl.when(j < x)
            def _(j=j):
                ent_v[...] = ent_v[...] * jnp.exp(lx_v[j]) + xr_v[j].astype(F32)
        enter = ent_v[...]
        log = jnp.zeros((1, DK), F32)
        for j in range(nz):
            zb_v[j] = (pre_v[j] + enter * jnp.exp(log)).astype(BF16)
            log = log + lz_v[j]
        for d in far_first(nz):
            b_copies[d].start()
        inc_v[z] = zb_v[z]
        f_copies[0].start()

    mark("w_b")

    @pl.when(c == 1)
    def _():
        for d in near_first(nz):
            b_copies[d].wait_recv()
            f_copies[d].start()

    mark("weights")
    ahead = 2

    @pl.when(c == 0)
    def _():
        for k in range(parts):
            pass_near(k)
            if k >= ahead:
                pass_far(k - ahead)

    mark("w_f")

    @pl.when(c == 0)
    def _():
        f_all.wait_recv()

    mark("gated")
    side_tok = tok // 2
    chunks = side_tok // 2 // SPAN
    order = [(s, j) for j in range(chunks) for s in (0, 1)]

    def start_row(s, own, j):
        lead = jnp.where(s == 0, ((y + 1) // 2) % 2, y // 2)
        lead = lead if own else 1 - lead
        return pl.multiple_of(s * side_tok + lead * (side_tok // 2) + j * SPAN, SPAN)

    def gated_rows(s, own, j):
        rows = pl.ds(start_row(s, own, j), SPAN)
        att = loc_v[rows, :] + mm_nt(qp_v[rows, :], inc_v[...].reshape(DV, DK))
        spread = jnp.mean(att * att, axis=-1, keepdims=True)
        return (att * lax.rsqrt(spread + 1e-05) * gate_v[rows, :]).astype(BF16)

    g_copies, r_copies, n_copies = [], [], []
    for s, j in order:
        gs_v[s, j] = gated_rows(s, False, j)
        g_copies.append(remote(gs_v.at[s, j], gr_v.at[s, j], g_sem.at[chunks * 2],
                               g_sem.at[s * chunks + j], {Y: near_of(s, y)}))
        g_copies[-1].start()
        r_copies.append(remote(rs_v.at[s, j], rr_v.at[s, j], r_sem.at[chunks * 2],
                               r_sem.at[s * chunks + j], {Y: far_of(s, y)}))
        n_copies.append(remote(fs_v.at[s, j], fr_v.at[s, j], n_sem.at[chunks * 2],
                               n_sem.at[s * chunks + j], {Y: near_of(s, y)}))
    for s, j in order:
        gm_v[s, j] = gated_rows(s, True, j)

    mark("w_weights")

    def arrive(i):
        both = wn_v.at[0]
        remote(both, both, wc_sem.at[0], wc_sem.at[1 + i], other).wait_recv()

    @pl.when(c == 1)
    def _():
        arrive(0)

    mark("proj")

    def pair_sum(s, j, block):
        cols = columns(block)
        return mm(gm_v[s, j], w_v[:, cols]) + mm(gr_v[s, j], wn_v[s, :, cols])

    for i, (s, j) in enumerate(order):
        far = far_of(s, y)
        mark(f"w_gather{i}")
        g_copies[i].wait_recv()
        mark(f"proj{i}")
        rs_v[s, j, 0] = pair_sum(s, j, far).astype(BF16)
        rs_v[s, j, 1] = pair_sum(s, j, near_of(s, far)).astype(BF16)
        r_copies[i].start()
        if i < ahead:
            mark(f"w_far{i}")

            @pl.when(c == 0)
            def _(i=i):
                pass_far(parts - ahead + i)

    mark("w_weights2")

    @pl.when(c == 1)
    def _():
        arrive(1)

    mark("keep")
    for s, j in order:
        k1_v[s, j] = pair_sum(s, j, near_of(s, y))
        k0_v[s, j] = pair_sum(s, j, y)
    mark("sum")

    def put(src, row):
        pltpu.make_async_copy(src, out_hbm.at[pl.ds(row, SPAN), :], out_sem.at[0]).start()

    for i, (s, j) in enumerate(order):
        mark(f"w_r{i}")
        r_copies[i].wait_recv()
        mark(f"sum{i}")
        fs_v[s, j] = (k1_v[s, j] + rr_v[s, j, 1].astype(F32)).astype(BF16)
        n_copies[i].start()
        o_v[s, j] = (k0_v[s, j] + rr_v[s, j, 0].astype(F32)).astype(BF16)
        put(o_v.at[s, j], start_row(s, True, j))
    mark("last")
    for i, (s, j) in enumerate(order):
        mark(f"w_n{i}")
        n_copies[i].wait_recv()
        put(fr_v.at[s, j], start_row(s, False, j))

    mark("drain")

    @pl.when(c == 0)
    def _():
        e_copy.wait_send()
        s_copy.wait_send()

        one = wn_v.at[0]
        for sem in (wy_sem, wx_sem):
            remote(one, one, sem.at[0], sem.at[1], other).wait_send()
        remote(wn_v, wn_v, wc_sem.at[0], wc_sem.at[1], other).wait_send()

    @pl.when(c == 1)
    def _():
        for copy in (lz_all, z_all, b_all, f_all):
            copy.wait_send()
        for d in range(1, nx):
            pl.when(x + d < nx)(lx_copies[d].wait_send)
            pl.when(x + d < nx)(x_copies[d].wait_send)

    for buf, sem in ((gs_v, g_sem), (rs_v, r_sem), (fs_v, n_sem)):
        remote(buf, buf, sem.at[chunks * 2], sem.at[0], other).wait_send()
    pltpu.make_async_copy(v_v, out_hbm, out_sem.at[0]).wait()
    mark(None)


def shards(nx, nz, queries, key_vectors, values, log_gate, out_gate, norm_gain, out_weight):
    tok = queries.shape[0]
    width = out_weight.shape[1] // 4
    piece = DV // nz
    chunks = tok // 4 // SPAN
    any_spec = pl.BlockSpec(memory_space=pl.ANY)
    vmem, dma = pltpu.VMEM, pltpu.SemaphoreType.DMA
    row = (tok, DK)
    weights = vmem(out_weight.shape, BF16)
    blocks = (2, chunks, SPAN, width)
    scratch = [
        vmem(row, BF16), vmem(row, BF16), vmem((tok, DV), BF16), vmem(row, BF16),
        vmem((tok, DV), BF16), vmem((1, DV), F32), weights, vmem((2,) + out_weight.shape, BF16),
        vmem(row, F32), vmem(row, BF16), vmem(row, BF16), vmem(row, BF16), vmem(row, BF16),
        vmem(row, BF16), vmem(row, BF16), vmem(row, BF16), vmem(row, BF16),
        vmem((tok, 256), BF16), vmem((256, 256), BF16), vmem((tok, DV), F32), vmem((tok, DV), F32),
        vmem((1, DK), F32), vmem((1, DK), F32),
        vmem((DV, DK), BF16), vmem((DV, DK), BF16), vmem((DV, DK), F32),
        vmem((1, DK), F32), vmem((nz, 1, DK), F32),
        vmem((nz, piece, DK), BF16), vmem((nz, piece, DK), BF16), vmem((nz, piece, DK), F32),
        vmem((1, DK), F32), vmem((nx, 1, DK), F32),
        vmem((piece, DK), BF16), vmem((nx, piece, DK), BF16), vmem((piece, DK), F32),
        vmem((nz, piece, DK), BF16), vmem((nz, piece, DK), BF16),
        vmem(blocks, BF16), vmem(blocks, BF16), vmem(blocks, BF16),
        vmem((2, chunks, 2, SPAN, width), BF16), vmem((2, chunks, 2, SPAN, width), BF16),
        vmem(blocks, F32), vmem(blocks, F32),
        vmem(blocks, BF16), vmem(blocks, BF16), vmem(blocks, BF16),
        dma((7,)), dma((1,)), dma((2,)), dma((2,)), dma((2,)), dma((2,)),
        dma((2, nx - 1)), dma((2, nx - 1)), dma((nz,)), dma((2,)),
        dma((5,)), dma((5,)), dma((3,)),
        dma((2 * chunks + 1,)), dma((2 * chunks + 1,)), dma((2 * chunks + 1,)),
    ]
    return pl.pallas_call(
        functools.partial(body, nx, nz, tok, width),
        out_shape=jax.ShapeDtypeStruct((tok, width), BF16),
        in_specs=[any_spec] * 7,
        out_specs=any_spec,
        scratch_shapes=scratch,
        compiler_params=pltpu.CompilerParams(
            collective_id=0, has_side_effects=True, vmem_limit_bytes=67043328
        ),
    )(queries, key_vectors, values, log_gate, out_gate, norm_gain.reshape(1, DV), out_weight)


def build(devices, nx, nz):
    split = Mesh(devices.reshape(nx, nz, 2, 4), (X, Z, C, Y))
    in_specs = (P(SEQ, Y),) * 5 + (P(Y), P(Y, None))
    return jax.shard_map(
        functools.partial(shards, nx, nz),
        mesh=split, in_specs=in_specs, out_specs=P(SEQ, Y), check_vma=False,
    )


def solution(mesh):
    return build(mesh.devices, 4, mesh.shape["seq"] // 8)
```

```python
import functools

import jax
import jax.numpy as jnp
from jax import lax
from jax.experimental import pallas as pl
from jax.experimental.pallas import tpu as pltpu
from jax.sharding import Mesh
from jax.sharding import PartitionSpec as P

DK = 256
DV = 512
SPAN = 64
X, Z, C, Y = ("seq_0", "seq_1", "seq_2", "head")
SEQ = (X, Z, C)
F32 = jnp.float32
BF16 = jnp.bfloat16
MESH_ID = pl.DeviceIdType.MESH
PROFILE = False


class Marks:
    def __init__(self):
        self.open = None

    def __call__(self, name):
        if not PROFILE:
            return
        if self.open is not None:
            self.open.__exit__(None, None, None)
        self.open = None
        if name:
            self.open = jax.named_scope(name)
            self.open.__enter__()


def mm(a, b):
    return lax.dot_general(a, b, (((1,), (0,)), ((), ())), preferred_element_type=F32)


def mm_nt(a, b):
    return lax.dot_general(a, b, (((1,), (1,)), ((), ())), preferred_element_type=F32)


def mm_tn(a, b):
    return lax.dot_general(a, b, (((0,), (0,)), ((), ())), preferred_element_type=F32)


def remote(src, dst, send, recv, where):
    return pltpu.make_async_remote_copy(
        src_ref=src, dst_ref=dst, send_sem=send, recv_sem=recv,
        device_id=where, device_id_type=MESH_ID,
    )


def far_first(n):
    return sorted(range(1, n), key=lambda d: (-min(d, n - d), d))


def near_first(n):
    return sorted(range(1, n), key=lambda d: (min(d, n - d), d))


def body(
    nx, nz, tok, width,
    q_hbm, k_hbm, v_hbm, g_hbm, og_hbm, gain_hbm, w_hbm, out_ref,
    q_v, k_v, v_v, g_v, og_v, gain_v, w_v, wn_v,
    run_v, kd_v, qa_v, ka_v, b_v, c_v, d_v, q0_v, qp_v, wgt_v, wd_v, loc_v, gate_v,
    es_v, er_v, ss_v, sr_v, own_v,
    lzs_v, lz_v, zs_v, zr_v, pre_v, lxs_v, lx_v, xs_v, xr_v, ent_v, zb_v, inc_v,
    gs_v, gr_v, gm_v, rs_v, rr_v, k0_v, k1_v, fs_v, fr_v,
    in_sem, e_sem, s_sem, lz_sem, z_sem, lx_sem, x_sem, b_sem, f_sem,
    wy_sem, wx_sem, wc_sem, g_sem, r_sem, n_sem,
):
    mark = Marks()
    x, z, c, y = (lax.axis_index(n) for n in (X, Z, C, Y))
    half = DV // 2
    piece = DV // nz
    y_a = y + 1 - 2 * (y % 2)
    y_b = 3 - y
    other = {C: 1 - c}
    z_to = [(z + d) % nz for d in range(nz)]
    z_from = [(z + nz - d) % nz for d in range(nz)]
    x_to = [(x + d) % nx for d in range(nx)]
    x_left = (x + nx - 1) % nx
    x_right = (x + 1) % nx

    e_copy = remote(es_v, er_v, e_sem.at[0], e_sem.at[1], other)
    s_copy = remote(ss_v, sr_v, s_sem.at[0], s_sem.at[1], other)
    most = pl.ds(0, nz - 1)
    lz_copies = {d: remote(lzs_v, lz_v.at[z], lz_sem.at[0], lz_sem.at[1], {Z: z_to[d]})
                 for d in range(1, nz)}
    lz_all = remote(lz_v.at[most], lz_v.at[most], lz_sem.at[0], lz_sem.at[1], other)
    z_copies = {d: remote(zs_v.at[z_to[d]], zr_v.at[z], z_sem.at[0], z_sem.at[1],
                          {Z: z_to[d]}) for d in range(1, nz)}
    z_all = remote(zs_v.at[most], zr_v.at[most], z_sem.at[0], z_sem.at[1], other)
    lx_copies = {d: remote(lxs_v, lx_v.at[x], lx_sem.at[0, d - 1], lx_sem.at[1, d - 1],
                           {X: x_to[d]}) for d in range(1, nx)}
    x_copies = {d: remote(xs_v, xr_v.at[x], x_sem.at[0, d - 1], x_sem.at[1, d - 1],
                          {X: x_to[d]}) for d in range(1, nx)}
    b_copies = {d: remote(zb_v.at[z_to[d]], inc_v.at[z], b_sem.at[0], b_sem.at[d],
                          {Z: z_to[d]}) for d in range(1, nz)}
    b_to = [remote(zb_v.at[j], inc_v.at[z], b_sem.at[0], b_sem.at[(j + nz - z) % nz], {Z: j})
            for j in range(nz)]
    b_all = remote(zb_v.at[most], inc_v.at[most], b_sem.at[0], b_sem.at[1], other)
    f_copies = {d: remote(inc_v.at[z_from[d]], inc_v.at[z_from[d]], f_sem.at[0],
                          f_sem.at[1], other) for d in range(nz)}
    f_all = remote(inc_v, inc_v, f_sem.at[0], f_sem.at[1], other)

    def step_a(v):
        return v + 1 - 2 * (v % 2)

    def near_of(s, v):
        return jnp.where(s == 0, step_a(v), 3 - v)

    def far_of(s, v):
        return jnp.where(s == 0, 3 - v, step_a(v))

    def columns(block):
        return pl.ds(pl.multiple_of(block * width, width), width)

    parts = 4
    step = DV // 2

    def w_part(s, owner, parity, k):
        far = far_of(s, owner)
        block = (far, near_of(s, far), near_of(s, owner), owner)[k]
        return pl.ds(pl.multiple_of(parity * step, step), step), columns(block)

    near_half, far_half = x % 2, 1 - x % 2

    def wy(s, k):
        to = near_of(s, y)
        rows, cols = w_part(s, to, near_half, k)
        return remote(w_v.at[rows, cols], wn_v.at[s, rows, cols], wy_sem.at[0], wy_sem.at[1 + k],
                      {Y: to})

    def passed(s, k, parity, send, recv, to):
        rows, cols = w_part(s, y, parity, k)
        buf = wn_v.at[s, rows, cols]
        return remote(buf, buf, send, recv, to)

    def wx(s, k):
        return passed(s, k, near_half, wx_sem.at[0], wx_sem.at[1 + k], {X: (x_left, x_right)[s]})

    def wc(s, k):
        return passed(s, k, near_half, wc_sem.at[0], wc_sem.at[1 + k // 2], other)

    def wd(s, k):
        return passed(s, k, far_half, wc_sem.at[0], wc_sem.at[1 + k // 2], other)

    def part_wait(sem, k):
        two = wn_v.at[:, pl.ds(0, step), pl.ds(0, width)]
        remote(two, two, sem.at[0], sem.at[1 + k], other).wait_recv()

    def pass_near(k):
        part_wait(wy_sem, k)
        for s in range(2):
            wx(s, k).start()
            wc(s, k).start()

    def pass_far(k):
        part_wait(wx_sem, k)
        for s in range(2):
            wd(s, k).start()

    def repeat(low, high, f):
        def one(k, _):
            f(k)
            return 0

        lax.fori_loop(low, high, one, 0)

    barrier = pltpu.get_barrier_semaphore()

    def greet(peers):
        for peer in peers:
            pl.semaphore_signal(barrier, inc=1, device_id=peer, device_id_type=MESH_ID)

    greet([other, {Y: y_a}, {Y: y_b}])

    @pl.when(c == 0)
    def _():
        greet([{X: x_left}, {X: x_right}])

    @pl.when(c == 1)
    def _():
        greet([{Z: z_to[d]} for d in range(1, nz)] + [{X: x_to[d]} for d in range(1, nx)])

    loads = []
    for i, (src, dst) in enumerate((
        (g_hbm, g_v), (k_hbm, k_v), (v_hbm, v_v), (w_hbm, w_v), (q_hbm, q_v),
        (og_hbm, og_v), (gain_hbm, gain_v),
    )):
        copy = pltpu.make_async_copy(src, dst, in_sem.at[i])
        copy.start()
        loads.append(copy)
    load_g, load_k, load_v, load_w, load_q, load_og, load_gain = loads

    group = 256
    tri = (
        lax.broadcasted_iota(jnp.int32, (group, group), 0)
        >= lax.broadcasted_iota(jnp.int32, (group, group), 1)
    ).astype(BF16)
    mark("w_g")
    load_g.wait()
    mark("cumsum")
    carry = jnp.zeros((1, DK), F32)
    for h in range(tok // group):
        rows = slice(h * group, (h + 1) * group)
        part = mm(tri, g_v[rows, :]) + carry
        run_v[rows, :] = part
        carry = part[group - 1:group, :]
    total = carry
    es_v[...] = total

    mark("keys")
    load_k.wait()

    def scale_keys(i):
        rows = pl.ds(pl.multiple_of(i * SPAN, SPAN), SPAN)
        kd_v[rows, :] = (k_v[rows, :].astype(F32) * jnp.exp(total - run_v[rows, :])).astype(BF16)

    repeat(0, tok // SPAN, scale_keys)
    mark("state")
    load_v.wait()
    for e in range(2):
        rows = slice(e * half, (e + 1) * half)
        own_v[rows, :] = mm_tn(v_v[:, rows], kd_v[...])
        ss_v[rows, :] = own_v[rows, :].astype(BF16)

    mark("w_barrier")

    @pl.when(c == 0)
    def _():
        pl.semaphore_wait(barrier, 5)
        e_copy.start()
        s_copy.start()
        load_w.wait()
        for k in range(parts):
            for s in range(2):
                wy(s, k).start()
        er_v[...] = jnp.zeros_like(er_v)

    @pl.when(c == 1)
    def _():
        pl.semaphore_wait(barrier, 3 + nz - 1 + nx - 1)

    mark("w_e")

    @pl.when(c == 1)
    def _():
        e_copy.wait_recv()
        lzs_v[...] = total + er_v[...]
        lz_v[z] = lzs_v[...]
        for d in far_first(nz):
            lz_copies[d].start()

    early = er_v[...]
    mark("w_s")

    @pl.when(c == 1)
    def _():
        s_copy.wait_recv()

    mark("chip_state")

    @pl.when(c == 1)
    def _():
        decay = jnp.exp(total)
        for j in range(nz):
            rows = slice(j * piece, (j + 1) * piece)
            zs_v[j] = (own_v[rows, :] + sr_v[rows, :].astype(F32) * decay).astype(BF16)
        for d in far_first(nz):
            z_copies[d].start()
        zr_v[z] = zs_v[z]
        load_w.wait()

    mark("scale_pair")
    load_q.wait()

    def scale_pair(i):
        rows = pl.ds(pl.multiple_of(i * SPAN, SPAN), SPAN)
        r = run_v[rows, :]
        mid = run_v[pl.ds(pl.multiple_of(i * SPAN + SPAN // 2, 8), 1), :]
        q = q_v[rows, :].astype(F32)
        k = k_v[rows, :].astype(F32)
        qa_v[rows, :] = (q * jnp.exp(r - mid)).astype(BF16)
        ka_v[rows, :] = (k * jnp.exp(mid - r)).astype(BF16)
        q0_v[rows, :] = (q * jnp.exp(r)).astype(BF16)
        qp_v[rows, :] = (q * jnp.exp(r + early)).astype(BF16)

    repeat(0, tok // SPAN, scale_pair)

    mark("scale_cross")
    for h, ref in ((SPAN, b_v), (2 * SPAN, c_v), (4 * SPAN, d_v)):
        for start in range(0, tok, 2 * h):
            edge = run_v[start + h - 1:start + h, :]

            def scale_cross(i, start=start, h=h, ref=ref, edge=edge):
                ke = pl.ds(pl.multiple_of(start + i * SPAN, SPAN), SPAN)
                qe = pl.ds(pl.multiple_of(start + h + i * SPAN, SPAN), SPAN)
                ref[ke, :] = (k_v[ke, :].astype(F32) * jnp.exp(edge - run_v[ke, :])).astype(BF16)
                ref[qe, :] = (q_v[qe, :].astype(F32) * jnp.exp(run_v[qe, :] - edge)).astype(BF16)

            repeat(0, h // SPAN, scale_cross)

    mark("attn")
    wide = 2 * SPAN
    ti = lax.broadcasted_iota(jnp.int32, (wide, wide), 0)
    si = lax.broadcasted_iota(jnp.int32, (wide, wide), 1)
    same = (ti // SPAN) == (si // SPAN)
    causal = same & (ti >= si)
    across = (ti // SPAN) > (si // SPAN)
    for m in range(tok // wide):
        rows = slice(m * wide, (m + 1) * wide)
        inside = mm_nt(qa_v[rows, :], ka_v[rows, :])
        between = mm_nt(b_v[rows, :], b_v[rows, :])
        diag = jnp.where(causal, inside, jnp.where(across, between, 0.0)).astype(BF16)
        if m % 2 == 0:
            wgt_v[rows, 0:wide] = diag
            wgt_v[rows, wide:2 * wide] = jnp.zeros_like(diag)
        else:
            before = slice((m - 1) * wide, m * wide)
            wgt_v[rows, 0:wide] = mm_nt(c_v[rows, :], c_v[before, :]).astype(BF16)
            wgt_v[rows, wide:2 * wide] = diag
    wd_v[...] = mm_nt(d_v[group:2 * group, :], d_v[0:group, :]).astype(BF16)
    for h in range(2):
        rows = slice(h * group, (h + 1) * group)
        acc = mm(wgt_v[rows, :], v_v[rows, :])
        if h:
            acc = acc + mm(wd_v[...], v_v[0:group, :])
        loc_v[rows, :] = acc

    @pl.when(c == 1)
    def _():
        for h in range(2):
            rows = slice(h * group, (h + 1) * group)
            loc_v[rows, :] = loc_v[rows, :] + mm_nt(q0_v[rows, :], sr_v[...])

    mark("gate")
    load_og.wait()
    load_gain.wait()

    def gate_rows(i):
        rows = pl.ds(pl.multiple_of(i * SPAN, SPAN), SPAN)
        u = og_v[rows, :].astype(F32)
        gate_v[rows, :] = gain_v[...] * (u / (1.0 + jnp.exp(-u)))

    repeat(0, tok // SPAN, gate_rows)

    mark("w_lz")

    @pl.when(c == 1)
    def _():
        lz_all.wait_recv()
        slab = lz_v[0]
        for j in range(1, nz):
            slab = slab + lz_v[j]
        lxs_v[...] = slab
        for d in range(1, nx):
            pl.when(x + d < nx)(lx_copies[d].start)

    mark("w_z")

    @pl.when(c == 1)
    def _():
        z_all.wait_recv()

    mark("zprefix")

    @pl.when(c == 1)
    def _():
        run = jnp.zeros((piece, DK), F32)
        for j in range(nz):
            pre_v[j] = run
            run = run * jnp.exp(lz_v[j]) + zr_v[j].astype(F32)
        xs_v[...] = run.astype(BF16)
        for d in far_first(nx):
            pl.when(x + d < nx)(x_copies[d].start)

    mark("w_x")

    @pl.when(c == 1)
    def _():
        for d in range(1, nx):
            pl.when(x >= d)(lx_copies[d].wait_recv)
        for d in near_first(nx):
            pl.when(x >= d)(x_copies[d].wait_recv)

    mark("xprefix")

    @pl.when(c == 1)
    def _():
        ent_v[...] = jnp.zeros_like(ent_v)
        for j in range(nx - 1):
            @pl.when(j < x)
            def _(j=j):
                ent_v[...] = ent_v[...] * jnp.exp(lx_v[j]) + xr_v[j].astype(F32)
        enter = ent_v[...]
        log = jnp.zeros((1, DK), F32)
        for j in range(nz):
            zb_v[j] = (pre_v[j] + enter * jnp.exp(log)).astype(BF16)
            log = log + lz_v[j]
        for j in range(nz):
            pl.when(z != j)(b_to[j].start)
        inc_v[z] = zb_v[z]
        f_copies[0].start()

    mark("w_b")

    @pl.when(c == 1)
    def _():
        for d in near_first(nz):
            b_copies[d].wait_recv()
            f_copies[d].start()

    mark("weights")
    ahead = 2

    @pl.when(c == 0)
    def _():
        for k in range(parts):
            pass_near(k)
            if k >= ahead:
                pass_far(k - ahead)

    mark("w_f")

    @pl.when(c == 0)
    def _():
        f_all.wait_recv()

    mark("gated")
    side_tok = tok // 2
    chunks = side_tok // 2 // SPAN
    order = [(s, j) for j in range(chunks) for s in (0, 1)]

    def start_row(s, own, j):
        lead = jnp.where(s == 0, ((y + 1) // 2) % 2, y // 2)
        lead = lead if own else 1 - lead
        return pl.multiple_of(s * side_tok + lead * (side_tok // 2) + j * SPAN, SPAN)

    def gated_rows(s, own, j):
        rows = pl.ds(start_row(s, own, j), SPAN)
        att = loc_v[rows, :] + mm_nt(qp_v[rows, :], inc_v[...].reshape(DV, DK))
        spread = jnp.mean(att * att, axis=-1, keepdims=True)
        return (att * lax.rsqrt(spread + 1e-05) * gate_v[rows, :]).astype(BF16)

    g_copies, r_copies, n_copies = [], [], []
    for s, j in order:
        gs_v[s, j] = gated_rows(s, False, j)
        g_copies.append(remote(gs_v.at[s, j], gr_v.at[s, j], g_sem.at[chunks * 2],
                               g_sem.at[s * chunks + j], {Y: near_of(s, y)}))
        g_copies[-1].start()
        r_copies.append(remote(rs_v.at[s, j], rr_v.at[s, j], r_sem.at[chunks * 2],
                               r_sem.at[s * chunks + j], {Y: far_of(s, y)}))
        n_copies.append(remote(fs_v.at[s, j], fr_v.at[s, j], n_sem.at[chunks * 2],
                               n_sem.at[s * chunks + j], {Y: near_of(s, y)}))
    for s, j in order:
        gm_v[s, j] = gated_rows(s, True, j)

    mark("w_weights")

    def arrive(i):
        both = wn_v.at[0]
        remote(both, both, wc_sem.at[0], wc_sem.at[1 + i], other).wait_recv()

    @pl.when(c == 1)
    def _():
        arrive(0)

    mark("proj")

    def pair_sum(s, j, block):
        cols = columns(block)
        return mm(gm_v[s, j], w_v[:, cols]) + mm(gr_v[s, j], wn_v[s, :, cols])

    for i, (s, j) in enumerate(order):
        far = far_of(s, y)
        mark(f"w_gather{i}")
        g_copies[i].wait_recv()
        mark(f"proj{i}")
        rs_v[s, j, 0] = pair_sum(s, j, far).astype(BF16)
        rs_v[s, j, 1] = pair_sum(s, j, near_of(s, far)).astype(BF16)
        r_copies[i].start()
        if i < ahead:
            mark(f"w_far{i}")

            @pl.when(c == 0)
            def _(i=i):
                pass_far(parts - ahead + i)

    mark("w_weights2")

    @pl.when(c == 1)
    def _():
        arrive(1)

    mark("keep")
    for s, j in order:
        k1_v[s, j] = pair_sum(s, j, near_of(s, y))
        k0_v[s, j] = pair_sum(s, j, y)
    mark("sum")

    for i, (s, j) in enumerate(order):
        mark(f"w_r{i}")
        r_copies[i].wait_recv()
        mark(f"sum{i}")
        fs_v[s, j] = (k1_v[s, j] + rr_v[s, j, 1].astype(F32)).astype(BF16)
        n_copies[i].start()
        out_ref[pl.ds(start_row(s, True, j), SPAN), :] = (
            k0_v[s, j] + rr_v[s, j, 0].astype(F32)
        ).astype(BF16)
    mark("last")
    for i, (s, j) in enumerate(order):
        mark(f"w_n{i}")
        n_copies[i].wait_recv()
        out_ref[pl.ds(start_row(s, False, j), SPAN), :] = fr_v[s, j]

    mark("drain")

    @pl.when(c == 0)
    def _():
        e_copy.wait_send()
        s_copy.wait_send()

        one = wn_v.at[0]
        for sem in (wy_sem, wx_sem):
            remote(one, one, sem.at[0], sem.at[1], other).wait_send()
        remote(wn_v, wn_v, wc_sem.at[0], wc_sem.at[1], other).wait_send()

    @pl.when(c == 1)
    def _():
        for copy in (lz_all, z_all, b_all, f_all):
            copy.wait_send()
        for d in range(1, nx):
            pl.when(x + d < nx)(lx_copies[d].wait_send)
            pl.when(x + d < nx)(x_copies[d].wait_send)

    for buf, sem in ((gs_v, g_sem), (rs_v, r_sem), (fs_v, n_sem)):
        remote(buf, buf, sem.at[chunks * 2], sem.at[0], other).wait_send()
    mark(None)


def shards(nx, nz, queries, key_vectors, values, log_gate, out_gate, norm_gain, out_weight):
    tok = queries.shape[0]
    width = out_weight.shape[1] // 4
    piece = DV // nz
    chunks = tok // 4 // SPAN
    any_spec = pl.BlockSpec(memory_space=pl.ANY)
    vmem, dma = pltpu.VMEM, pltpu.SemaphoreType.DMA
    row = (tok, DK)
    weights = vmem(out_weight.shape, BF16)
    blocks = (2, chunks, SPAN, width)
    scratch = [
        vmem(row, BF16), vmem(row, BF16), vmem((tok, DV), BF16), vmem(row, BF16),
        vmem((tok, DV), BF16), vmem((1, DV), F32), weights, vmem((2,) + out_weight.shape, BF16),
        vmem(row, F32), vmem(row, BF16), vmem(row, BF16), vmem(row, BF16), vmem(row, BF16),
        vmem(row, BF16), vmem(row, BF16), vmem(row, BF16), vmem(row, BF16),
        vmem((tok, 256), BF16), vmem((256, 256), BF16), vmem((tok, DV), F32), vmem((tok, DV), F32),
        vmem((1, DK), F32), vmem((1, DK), F32),
        vmem((DV, DK), BF16), vmem((DV, DK), BF16), vmem((DV, DK), F32),
        vmem((1, DK), F32), vmem((nz, 1, DK), F32),
        vmem((nz, piece, DK), BF16), vmem((nz, piece, DK), BF16), vmem((nz, piece, DK), F32),
        vmem((1, DK), F32), vmem((nx, 1, DK), F32),
        vmem((piece, DK), BF16), vmem((nx, piece, DK), BF16), vmem((piece, DK), F32),
        vmem((nz, piece, DK), BF16), vmem((nz, piece, DK), BF16),
        vmem(blocks, BF16), vmem(blocks, BF16), vmem(blocks, BF16),
        vmem((2, chunks, 2, SPAN, width), BF16), vmem((2, chunks, 2, SPAN, width), BF16),
        vmem(blocks, F32), vmem(blocks, F32),
        vmem(blocks, BF16), vmem(blocks, BF16),
        dma((7,)), dma((2,)), dma((2,)), dma((2,)), dma((2,)),
        dma((2, nx - 1)), dma((2, nx - 1)), dma((nz,)), dma((2,)),
        dma((5,)), dma((5,)), dma((3,)),
        dma((2 * chunks + 1,)), dma((2 * chunks + 1,)), dma((2 * chunks + 1,)),
    ]
    return pl.pallas_call(
        functools.partial(body, nx, nz, tok, width),
        out_shape=jax.ShapeDtypeStruct((tok, width), BF16),
        in_specs=[any_spec] * 7,
        out_specs=pl.BlockSpec(memory_space=pltpu.VMEM),
        scratch_shapes=scratch,
        compiler_params=pltpu.CompilerParams(
            collective_id=0, has_side_effects=True, vmem_limit_bytes=40 * 2**20
        ),
    )(*[pltpu.with_memory_space_constraint(v, pltpu.HBM) for v in (
        queries, key_vectors, values, log_gate, out_gate, norm_gain.reshape(1, DV), out_weight)])


def build(devices, nx, nz):
    split = Mesh(devices.reshape(nx, nz, 2, 4), (X, Z, C, Y))
    in_specs = (P(SEQ, Y),) * 5 + (P(Y), P(Y, None))
    return jax.shard_map(
        functools.partial(shards, nx, nz),
        mesh=split, in_specs=in_specs, out_specs=P(SEQ, Y), check_vma=False,
    )


def solution(mesh):
    return build(mesh.devices, 4, mesh.shape["seq"] // 8)
```

```python
import functools

import jax
import jax.numpy as jnp
from jax import lax
from jax.experimental import pallas as pl
from jax.experimental.pallas import tpu as pltpu
from jax.sharding import Mesh
from jax.sharding import PartitionSpec as P

DK = 256
DV = 512
SPAN = 64
X, Z, C, Y = ("seq_0", "seq_1", "seq_2", "head")
SEQ = (X, Z, C)
F32 = jnp.float32
BF16 = jnp.bfloat16
MESH_ID = pl.DeviceIdType.MESH
PROFILE = False


class Marks:
    def __init__(self):
        self.open = None

    def __call__(self, name):
        if not PROFILE:
            return
        if self.open is not None:
            self.open.__exit__(None, None, None)
        self.open = None
        if name:
            self.open = jax.named_scope(name)
            self.open.__enter__()


def mm(a, b):
    return lax.dot_general(a, b, (((1,), (0,)), ((), ())), preferred_element_type=F32)


def mm_nt(a, b):
    return lax.dot_general(a, b, (((1,), (1,)), ((), ())), preferred_element_type=F32)


def mm_tn(a, b):
    return lax.dot_general(a, b, (((0,), (0,)), ((), ())), preferred_element_type=F32)


def remote(src, dst, send, recv, where):
    return pltpu.make_async_remote_copy(
        src_ref=src, dst_ref=dst, send_sem=send, recv_sem=recv,
        device_id=where, device_id_type=MESH_ID,
    )


def far_first(n):
    return sorted(range(1, n), key=lambda d: (-min(d, n - d), d))


def near_first(n):
    return sorted(range(1, n), key=lambda d: (min(d, n - d), d))


def body(
    nx, nz, tok, width,
    q_hbm, k_hbm, v_hbm, g_hbm, og_hbm, gain_hbm, w_hbm, out_ref,
    q_v, k_v, v_v, g_v, og_v, gain_v, w_v, wn_v,
    run_v, kd_v, qa_v, ka_v, b_v, c_v, d_v, q0_v, qp_v, wgt_v, wd_v, loc_v, gate_v,
    es_v, er_v, ss_v, sr_v, own_v,
    lzs_v, lz_v, zs_v, zr_v, pre_v, lxs_v, lx_v, xs_v, xr_v, ent_v, zb_v, inc_v,
    gs_v, gr_v, gm_v, rs_v, rr_v, k0_v, k1_v, fs_v, fr_v,
    in_sem, e_sem, s_sem, lz_sem, z_sem, lx_sem, x_sem, b_sem, f_sem,
    wy_sem, wx_sem, wc_sem, g_sem, r_sem, n_sem,
):
    mark = Marks()
    x, z, c, y = (lax.axis_index(n) for n in (X, Z, C, Y))
    half = DV // 2
    piece = DV // nz
    y_a = y + 1 - 2 * (y % 2)
    y_b = 3 - y
    other = {C: 1 - c}
    z_to = [(z + d) % nz for d in range(nz)]
    z_from = [(z + nz - d) % nz for d in range(nz)]
    x_to = [(x + d) % nx for d in range(nx)]
    x_left = (x + nx - 1) % nx
    x_right = (x + 1) % nx

    e_copy = remote(es_v, er_v, e_sem.at[0], e_sem.at[1], other)
    s_copy = remote(ss_v, sr_v, s_sem.at[0], s_sem.at[1], other)
    most = pl.ds(0, nz - 1)
    lz_copies = {d: remote(lzs_v, lz_v.at[z], lz_sem.at[0], lz_sem.at[1], {Z: z_to[d]})
                 for d in range(1, nz)}
    lz_all = remote(lz_v.at[most], lz_v.at[most], lz_sem.at[0], lz_sem.at[1], other)
    z_copies = {d: remote(zs_v.at[z_to[d]], zr_v.at[z], z_sem.at[0], z_sem.at[1],
                          {Z: z_to[d]}) for d in range(1, nz)}
    z_all = remote(zs_v.at[most], zr_v.at[most], z_sem.at[0], z_sem.at[1], other)
    lx_copies = {d: remote(lxs_v, lx_v.at[x], lx_sem.at[0, d - 1], lx_sem.at[1, d - 1],
                           {X: x_to[d]}) for d in range(1, nx)}
    x_copies = {d: remote(xs_v, xr_v.at[x], x_sem.at[0, d - 1], x_sem.at[1, d - 1],
                          {X: x_to[d]}) for d in range(1, nx)}
    b_copies = {d: remote(zb_v.at[z_to[d]], inc_v.at[z], b_sem.at[0], b_sem.at[d],
                          {Z: z_to[d]}) for d in range(1, nz)}
    b_to = [remote(zb_v.at[j], inc_v.at[z], b_sem.at[0], b_sem.at[(j + nz - z) % nz], {Z: j})
            for j in range(nz)]
    b_all = remote(zb_v.at[most], inc_v.at[most], b_sem.at[0], b_sem.at[1], other)
    f_copies = {d: remote(inc_v.at[z_from[d]], inc_v.at[z_from[d]], f_sem.at[0],
                          f_sem.at[1], other) for d in range(nz)}
    f_all = remote(inc_v, inc_v, f_sem.at[0], f_sem.at[1], other)

    def step_a(v):
        return v + 1 - 2 * (v % 2)

    def near_of(s, v):
        return jnp.where(s == 0, step_a(v), 3 - v)

    def far_of(s, v):
        return jnp.where(s == 0, 3 - v, step_a(v))

    def columns(block):
        return pl.ds(pl.multiple_of(block * width, width), width)

    parts = 4
    step = DV // 2

    def w_part(s, owner, parity, k):
        far = far_of(s, owner)
        block = (far, near_of(s, far), near_of(s, owner), owner)[k]
        return pl.ds(pl.multiple_of(parity * step, step), step), columns(block)

    near_half, far_half = x % 2, 1 - x % 2

    def wy(s, k):
        to = near_of(s, y)
        rows, cols = w_part(s, to, near_half, k)
        return remote(w_v.at[rows, cols], wn_v.at[s, rows, cols], wy_sem.at[0], wy_sem.at[1 + k],
                      {Y: to})

    def passed(s, k, parity, send, recv, to):
        rows, cols = w_part(s, y, parity, k)
        buf = wn_v.at[s, rows, cols]
        return remote(buf, buf, send, recv, to)

    def wx(s, k):
        return passed(s, k, near_half, wx_sem.at[0], wx_sem.at[1 + k], {X: (x_left, x_right)[s]})

    def wc(s, k):
        return passed(s, k, near_half, wc_sem.at[0], wc_sem.at[1 + k // 2], other)

    def wd(s, k):
        return passed(s, k, far_half, wc_sem.at[0], wc_sem.at[1 + k // 2], other)

    def part_wait(sem, k):
        two = wn_v.at[:, pl.ds(0, step), pl.ds(0, width)]
        remote(two, two, sem.at[0], sem.at[1 + k], other).wait_recv()

    def pass_near(k):
        part_wait(wy_sem, k)
        for s in range(2):
            wx(s, k).start()
            wc(s, k).start()

    def pass_far(k):
        part_wait(wx_sem, k)
        for s in range(2):
            wd(s, k).start()

    def repeat(low, high, f):
        def one(k, _):
            f(k)
            return 0

        lax.fori_loop(low, high, one, 0)

    barrier = pltpu.get_barrier_semaphore()

    def greet(peers):
        for peer in peers:
            pl.semaphore_signal(barrier, inc=1, device_id=peer, device_id_type=MESH_ID)

    greet([other, {Y: y_a}, {Y: y_b}])

    @pl.when(c == 0)
    def _():
        greet([{X: x_left}, {X: x_right}])

    @pl.when(c == 1)
    def _():
        greet([{Z: z_to[d]} for d in range(1, nz)] + [{X: x_to[d]} for d in range(1, nx)])

    loads = []
    for i, (src, dst) in enumerate((
        (g_hbm, g_v), (k_hbm, k_v), (v_hbm, v_v), (w_hbm, w_v), (q_hbm, q_v),
        (og_hbm, og_v), (gain_hbm, gain_v),
    )):
        copy = pltpu.make_async_copy(src, dst, in_sem.at[i])
        copy.start()
        loads.append(copy)
    load_g, load_k, load_v, load_w, load_q, load_og, load_gain = loads

    group = 256
    tri = (
        lax.broadcasted_iota(jnp.int32, (group, group), 0)
        >= lax.broadcasted_iota(jnp.int32, (group, group), 1)
    ).astype(BF16)
    mark("w_g")
    load_g.wait()
    mark("cumsum")
    carry = jnp.zeros((1, DK), F32)
    for h in range(tok // group):
        rows = slice(h * group, (h + 1) * group)
        part = mm(tri, g_v[rows, :]) + carry
        run_v[rows, :] = part
        carry = part[group - 1:group, :]
    total = carry
    es_v[...] = total

    mark("keys")
    load_k.wait()

    def scale_keys(i):
        rows = pl.ds(pl.multiple_of(i * SPAN, SPAN), SPAN)
        kd_v[rows, :] = (k_v[rows, :].astype(F32) * jnp.exp(total - run_v[rows, :])).astype(BF16)

    repeat(0, tok // SPAN, scale_keys)
    mark("state")
    load_v.wait()
    for e in range(2):
        rows = slice(e * half, (e + 1) * half)
        own_v[rows, :] = mm_tn(v_v[:, rows], kd_v[...])
        ss_v[rows, :] = own_v[rows, :].astype(BF16)

    mark("w_barrier")

    @pl.when(c == 0)
    def _():
        pl.semaphore_wait(barrier, 5)
        e_copy.start()
        s_copy.start()
        load_w.wait()
        for k in range(parts):
            for s in range(2):
                wy(s, k).start()
        er_v[...] = jnp.zeros_like(er_v)

    @pl.when(c == 1)
    def _():
        pl.semaphore_wait(barrier, 3 + nz - 1 + nx - 1)

    mark("w_e")

    @pl.when(c == 1)
    def _():
        e_copy.wait_recv()
        lzs_v[...] = total + er_v[...]
        lz_v[z] = lzs_v[...]
        for d in far_first(nz):
            lz_copies[d].start()

    early = er_v[...]
    mark("w_s")

    @pl.when(c == 1)
    def _():
        s_copy.wait_recv()

    mark("chip_state")

    @pl.when(c == 1)
    def _():
        decay = jnp.exp(total)
        for j in range(nz):
            rows = slice(j * piece, (j + 1) * piece)
            zs_v[j] = (own_v[rows, :] + sr_v[rows, :].astype(F32) * decay).astype(BF16)
        for d in far_first(nz):
            z_copies[d].start()
        zr_v[z] = zs_v[z]
        load_w.wait()

    mark("scale_pair")
    load_q.wait()

    def scale_pair(i):
        rows = pl.ds(pl.multiple_of(i * SPAN, SPAN), SPAN)
        r = run_v[rows, :]
        mid = run_v[pl.ds(pl.multiple_of(i * SPAN + SPAN // 2, 8), 1), :]
        q = q_v[rows, :].astype(F32)
        k = k_v[rows, :].astype(F32)
        qa_v[rows, :] = (q * jnp.exp(r - mid)).astype(BF16)
        ka_v[rows, :] = (k * jnp.exp(mid - r)).astype(BF16)
        q0_v[rows, :] = (q * jnp.exp(r)).astype(BF16)
        qp_v[rows, :] = (q * jnp.exp(r + early)).astype(BF16)

    repeat(0, tok // SPAN, scale_pair)

    mark("scale_cross")
    for h, ref in ((SPAN, b_v), (2 * SPAN, c_v), (4 * SPAN, d_v)):
        for start in range(0, tok, 2 * h):
            edge = run_v[start + h - 1:start + h, :]

            def scale_cross(i, start=start, h=h, ref=ref, edge=edge):
                ke = pl.ds(pl.multiple_of(start + i * SPAN, SPAN), SPAN)
                qe = pl.ds(pl.multiple_of(start + h + i * SPAN, SPAN), SPAN)
                ref[ke, :] = (k_v[ke, :].astype(F32) * jnp.exp(edge - run_v[ke, :])).astype(BF16)
                ref[qe, :] = (q_v[qe, :].astype(F32) * jnp.exp(run_v[qe, :] - edge)).astype(BF16)

            repeat(0, h // SPAN, scale_cross)

    mark("attn")
    wide = 2 * SPAN
    ti = lax.broadcasted_iota(jnp.int32, (wide, wide), 0)
    si = lax.broadcasted_iota(jnp.int32, (wide, wide), 1)
    same = (ti // SPAN) == (si // SPAN)
    causal = same & (ti >= si)
    across = (ti // SPAN) > (si // SPAN)
    for m in range(tok // wide):
        rows = slice(m * wide, (m + 1) * wide)
        inside = mm_nt(qa_v[rows, :], ka_v[rows, :])
        between = mm_nt(b_v[rows, :], b_v[rows, :])
        diag = jnp.where(causal, inside, jnp.where(across, between, 0.0)).astype(BF16)
        if m % 2 == 0:
            wgt_v[rows, 0:wide] = diag
            wgt_v[rows, wide:2 * wide] = jnp.zeros_like(diag)
        else:
            before = slice((m - 1) * wide, m * wide)
            wgt_v[rows, 0:wide] = mm_nt(c_v[rows, :], c_v[before, :]).astype(BF16)
            wgt_v[rows, wide:2 * wide] = diag
    wd_v[...] = mm_nt(d_v[group:2 * group, :], d_v[0:group, :]).astype(BF16)
    for h in range(2):
        rows = slice(h * group, (h + 1) * group)
        acc = mm(wgt_v[rows, :], v_v[rows, :])
        if h:
            acc = acc + mm(wd_v[...], v_v[0:group, :])
        loc_v[rows, :] = acc

    @pl.when(c == 1)
    def _():
        for h in range(2):
            rows = slice(h * group, (h + 1) * group)
            loc_v[rows, :] = loc_v[rows, :] + mm_nt(q0_v[rows, :], sr_v[...])

    mark("gate")
    load_og.wait()
    load_gain.wait()

    def gate_rows(i):
        rows = pl.ds(pl.multiple_of(i * SPAN, SPAN), SPAN)
        u = og_v[rows, :].astype(F32)
        gate_v[rows, :] = gain_v[...] * (u / (1.0 + jnp.exp(-u)))

    repeat(0, tok // SPAN, gate_rows)

    mark("w_lz")

    @pl.when(c == 1)
    def _():
        lz_all.wait_recv()
        slab = lz_v[0]
        for j in range(1, nz):
            slab = slab + lz_v[j]
        lxs_v[...] = slab
        for d in range(1, nx):
            pl.when(x + d < nx)(lx_copies[d].start)

    mark("w_z")

    @pl.when(c == 1)
    def _():
        z_all.wait_recv()

    mark("zprefix")

    @pl.when(c == 1)
    def _():
        run = jnp.zeros((piece, DK), F32)
        for j in range(nz):
            pre_v[j] = run
            run = run * jnp.exp(lz_v[j]) + zr_v[j].astype(F32)
        xs_v[...] = run.astype(BF16)
        pl.when(x == 0)(x_copies[1].start)
        for d in far_first(nx):
            pl.when((x + d < nx) & ((x > 0) | (d > 1)))(x_copies[d].start)

    mark("w_x")

    @pl.when(c == 1)
    def _():
        for d in range(1, nx):
            pl.when(x >= d)(lx_copies[d].wait_recv)
        for d in near_first(nx):
            pl.when(x >= d)(x_copies[d].wait_recv)

    mark("xprefix")

    @pl.when(c == 1)
    def _():
        ent_v[...] = jnp.zeros_like(ent_v)
        for j in range(nx - 1):
            @pl.when(j < x)
            def _(j=j):
                ent_v[...] = ent_v[...] * jnp.exp(lx_v[j]) + xr_v[j].astype(F32)
        enter = ent_v[...]
        log = jnp.zeros((1, DK), F32)
        for j in range(nz):
            zb_v[j] = (pre_v[j] + enter * jnp.exp(log)).astype(BF16)
            log = log + lz_v[j]
        for j in range(nz):
            pl.when(z != j)(b_to[j].start)
        inc_v[z] = zb_v[z]
        f_copies[0].start()

    mark("w_b")

    @pl.when(c == 1)
    def _():
        for d in near_first(nz):
            b_copies[d].wait_recv()
            f_copies[d].start()

    mark("weights")
    ahead = 2

    @pl.when(c == 0)
    def _():
        for k in range(parts):
            pass_near(k)
            if k >= ahead:
                pass_far(k - ahead)

    mark("w_f")

    @pl.when(c == 0)
    def _():
        f_all.wait_recv()

    mark("gated")
    side_tok = tok // 2
    chunks = side_tok // 2 // SPAN
    order = [(s, j) for j in range(chunks) for s in (1, 0)]

    def start_row(s, own, j):
        lead = jnp.where(s == 0, ((y + 1) // 2) % 2, y // 2)
        lead = lead if own else 1 - lead
        return pl.multiple_of(s * side_tok + lead * (side_tok // 2) + j * SPAN, SPAN)

    def gated_rows(s, own, j):
        rows = pl.ds(start_row(s, own, j), SPAN)
        att = loc_v[rows, :] + mm_nt(qp_v[rows, :], inc_v[...].reshape(DV, DK))
        spread = jnp.mean(att * att, axis=-1, keepdims=True)
        return (att * lax.rsqrt(spread + 1e-05) * gate_v[rows, :]).astype(BF16)

    g_copies, r_copies, n_copies = [], [], []
    for s, j in order:
        gs_v[s, j] = gated_rows(s, False, j)
        g_copies.append(remote(gs_v.at[s, j], gr_v.at[s, j], g_sem.at[chunks * 2],
                               g_sem.at[s * chunks + j], {Y: near_of(s, y)}))
        g_copies[-1].start()
        r_copies.append(remote(rs_v.at[s, j], rr_v.at[s, j], r_sem.at[chunks * 2],
                               r_sem.at[s * chunks + j], {Y: far_of(s, y)}))
        n_copies.append(remote(fs_v.at[s, j], fr_v.at[s, j], n_sem.at[chunks * 2],
                               n_sem.at[s * chunks + j], {Y: near_of(s, y)}))
    for s, j in order:
        gm_v[s, j] = gated_rows(s, True, j)

    mark("w_weights")

    def arrive(i):
        both = wn_v.at[0]
        remote(both, both, wc_sem.at[0], wc_sem.at[1 + i], other).wait_recv()

    @pl.when(c == 1)
    def _():
        arrive(0)

    mark("proj")

    def pair_sum(s, j, block):
        cols = columns(block)
        return mm(gm_v[s, j], w_v[:, cols]) + mm(gr_v[s, j], wn_v[s, :, cols])

    for i, (s, j) in enumerate(order):
        far = far_of(s, y)
        mark(f"w_gather{i}")
        g_copies[i].wait_recv()
        mark(f"proj{i}")
        rs_v[s, j, 0] = pair_sum(s, j, far).astype(BF16)
        rs_v[s, j, 1] = pair_sum(s, j, near_of(s, far)).astype(BF16)
        r_copies[i].start()
        if i < ahead:
            mark(f"w_far{i}")

            @pl.when(c == 0)
            def _(i=i):
                pass_far(parts - ahead + i)

    mark("w_weights2")

    @pl.when(c == 1)
    def _():
        arrive(1)

    mark("keep")
    for s, j in order:
        k1_v[s, j] = pair_sum(s, j, near_of(s, y))
        k0_v[s, j] = pair_sum(s, j, y)
    mark("sum")

    for i, (s, j) in enumerate(order):
        mark(f"w_r{i}")
        r_copies[i].wait_recv()
        mark(f"sum{i}")
        fs_v[s, j] = (k1_v[s, j] + rr_v[s, j, 1].astype(F32)).astype(BF16)
        pl.when(c == 0)(n_copies[i].start)
        out_ref[pl.ds(start_row(s, True, j), SPAN), :] = (
            k0_v[s, j] + rr_v[s, j, 0].astype(F32)
        ).astype(BF16)
    mark("last")

    @pl.when(c == 1)
    def _():
        for copy in n_copies:
            copy.start()

    for i, (s, j) in enumerate(order):
        mark(f"w_n{i}")
        n_copies[i].wait_recv()
        out_ref[pl.ds(start_row(s, False, j), SPAN), :] = fr_v[s, j]

    mark("drain")

    @pl.when(c == 0)
    def _():
        e_copy.wait_send()
        s_copy.wait_send()

        one = wn_v.at[0]
        for sem in (wy_sem, wx_sem):
            remote(one, one, sem.at[0], sem.at[1], other).wait_send()
        remote(wn_v, wn_v, wc_sem.at[0], wc_sem.at[1], other).wait_send()

    @pl.when(c == 1)
    def _():
        for copy in (lz_all, z_all, b_all, f_all):
            copy.wait_send()
        for d in range(1, nx):
            pl.when(x + d < nx)(lx_copies[d].wait_send)
            pl.when(x + d < nx)(x_copies[d].wait_send)

    for buf, sem in ((gs_v, g_sem), (rs_v, r_sem), (fs_v, n_sem)):
        remote(buf, buf, sem.at[chunks * 2], sem.at[0], other).wait_send()
    mark(None)


def shards(nx, nz, queries, key_vectors, values, log_gate, out_gate, norm_gain, out_weight):
    tok = queries.shape[0]
    width = out_weight.shape[1] // 4
    piece = DV // nz
    chunks = tok // 4 // SPAN
    any_spec = pl.BlockSpec(memory_space=pl.ANY)
    vmem, dma = pltpu.VMEM, pltpu.SemaphoreType.DMA
    row = (tok, DK)
    weights = vmem(out_weight.shape, BF16)
    blocks = (2, chunks, SPAN, width)
    scratch = [
        vmem(row, BF16), vmem(row, BF16), vmem((tok, DV), BF16), vmem(row, BF16),
        vmem((tok, DV), BF16), vmem((1, DV), F32), weights, vmem((2,) + out_weight.shape, BF16),
        vmem(row, F32), vmem(row, BF16), vmem(row, BF16), vmem(row, BF16), vmem(row, BF16),
        vmem(row, BF16), vmem(row, BF16), vmem(row, BF16), vmem(row, BF16),
        vmem((tok, 256), BF16), vmem((256, 256), BF16), vmem((tok, DV), F32), vmem((tok, DV), F32),
        vmem((1, DK), F32), vmem((1, DK), F32),
        vmem((DV, DK), BF16), vmem((DV, DK), BF16), vmem((DV, DK), F32),
        vmem((1, DK), F32), vmem((nz, 1, DK), F32),
        vmem((nz, piece, DK), BF16), vmem((nz, piece, DK), BF16), vmem((nz, piece, DK), F32),
        vmem((1, DK), F32), vmem((nx, 1, DK), F32),
        vmem((piece, DK), BF16), vmem((nx, piece, DK), BF16), vmem((piece, DK), F32),
        vmem((nz, piece, DK), BF16), vmem((nz, piece, DK), BF16),
        vmem(blocks, BF16), vmem(blocks, BF16), vmem(blocks, BF16),
        vmem((2, chunks, 2, SPAN, width), BF16), vmem((2, chunks, 2, SPAN, width), BF16),
        vmem(blocks, F32), vmem(blocks, F32),
        vmem(blocks, BF16), vmem(blocks, BF16),
        dma((7,)), dma((2,)), dma((2,)), dma((2,)), dma((2,)),
        dma((2, nx - 1)), dma((2, nx - 1)), dma((nz,)), dma((2,)),
        dma((5,)), dma((5,)), dma((3,)),
        dma((2 * chunks + 1,)), dma((2 * chunks + 1,)), dma((2 * chunks + 1,)),
    ]
    return pl.pallas_call(
        functools.partial(body, nx, nz, tok, width),
        out_shape=jax.ShapeDtypeStruct((tok, width), BF16),
        in_specs=[any_spec] * 7,
        out_specs=pl.BlockSpec(memory_space=pltpu.VMEM),
        scratch_shapes=scratch,
        compiler_params=pltpu.CompilerParams(
            collective_id=0, has_side_effects=True, vmem_limit_bytes=40 * 2**20
        ),
    )(*[pltpu.with_memory_space_constraint(v, pltpu.HBM) for v in (
        queries, key_vectors, values, log_gate, out_gate, norm_gain.reshape(1, DV), out_weight)])


def build(devices, nx, nz):
    split = Mesh(devices.reshape(nx, nz, 2, 4), (X, Z, C, Y))
    in_specs = (P(SEQ, Y),) * 5 + (P(Y), P(Y, None))
    return jax.shard_map(
        functools.partial(shards, nx, nz),
        mesh=split, in_specs=in_specs, out_specs=P(SEQ, Y), check_vma=False,
    )


def solution(mesh):
    return build(mesh.devices, 4, mesh.shape["seq"] // 8)
```

```python
import functools

import jax
import jax.numpy as jnp
from jax import lax
from jax.experimental import pallas as pl
from jax.experimental.pallas import tpu as pltpu
from jax.sharding import Mesh
from jax.sharding import PartitionSpec as P

DK = 256
DV = 512
SPAN = 64
X, Z, C, Y = ("seq_0", "seq_1", "seq_2", "head")
SEQ = (X, Z, C)
F32 = jnp.float32
BF16 = jnp.bfloat16
MESH_ID = pl.DeviceIdType.MESH
PROFILE = False


class Marks:
    def __init__(self):
        self.open = None

    def __call__(self, name):
        if not PROFILE:
            return
        if self.open is not None:
            self.open.__exit__(None, None, None)
        self.open = None
        if name:
            self.open = jax.named_scope(name)
            self.open.__enter__()


def mm(a, b):
    return lax.dot_general(a, b, (((1,), (0,)), ((), ())), preferred_element_type=F32)


def mm_nt(a, b):
    return lax.dot_general(a, b, (((1,), (1,)), ((), ())), preferred_element_type=F32)


def mm_tn(a, b):
    return lax.dot_general(a, b, (((0,), (0,)), ((), ())), preferred_element_type=F32)


def remote(src, dst, send, recv, where):
    return pltpu.make_async_remote_copy(
        src_ref=src, dst_ref=dst, send_sem=send, recv_sem=recv,
        device_id=where, device_id_type=MESH_ID,
    )


def far_first(n):
    return sorted(range(1, n), key=lambda d: (-min(d, n - d), d))


def near_first(n):
    return sorted(range(1, n), key=lambda d: (min(d, n - d), d))


def body(
    nx, nz, tok, width,
    q_hbm, k_hbm, v_hbm, g_hbm, og_hbm, gain_hbm, w_hbm, out_ref,
    q_v, k_v, v_v, g_v, og_v, gain_v, w_v, wn_v,
    run_v, kd_v, qa_v, ka_v, b_v, c_v, d_v, q0_v, qp_v, wgt_v, wd_v, loc_v, gate_v,
    es_v, er_v, ss_v, sr_v, own_v,
    lzs_v, lz_v, zs_v, zr_v, pre_v, lxs_v, lx_v, xs_v, xr_v, ent_v, zb_v, inc_v,
    gs_v, gr_v, gm_v, rs_v, rr_v, k0_v, k1_v, fs_v, fr_v,
    in_sem, e_sem, s_sem, lz_sem, z_sem, lx_sem, x_sem, b_sem, f_sem,
    wy_sem, wx_sem, wc_sem, g_sem, r_sem, n_sem,
):
    mark = Marks()
    x, z, c, y = (lax.axis_index(n) for n in (X, Z, C, Y))
    half = DV // 2
    piece = DV // nz
    y_a = y + 1 - 2 * (y % 2)
    y_b = 3 - y
    other = {C: 1 - c}
    z_to = [(z + d) % nz for d in range(nz)]
    z_from = [(z + nz - d) % nz for d in range(nz)]
    x_to = [(x + d) % nx for d in range(nx)]
    x_left = (x + nx - 1) % nx
    x_right = (x + 1) % nx

    e_copy = remote(es_v, er_v, e_sem.at[0], e_sem.at[1], other)
    s_copy = remote(ss_v, sr_v, s_sem.at[0], s_sem.at[1], other)
    most = pl.ds(0, nz - 1)
    lz_copies = {d: remote(lzs_v, lz_v.at[z], lz_sem.at[0], lz_sem.at[1], {Z: z_to[d]})
                 for d in range(1, nz)}
    lz_all = remote(lz_v.at[most], lz_v.at[most], lz_sem.at[0], lz_sem.at[1], other)
    z_copies = {d: remote(zs_v.at[z_to[d]], zr_v.at[z], z_sem.at[0], z_sem.at[1],
                          {Z: z_to[d]}) for d in range(1, nz)}
    z_all = remote(zs_v.at[most], zr_v.at[most], z_sem.at[0], z_sem.at[1], other)
    lx_copies = {d: remote(lxs_v, lx_v.at[x], lx_sem.at[0, d - 1], lx_sem.at[1, d - 1],
                           {X: x_to[d]}) for d in range(1, nx)}
    x_copies = {d: remote(xs_v, xr_v.at[x], x_sem.at[0, d - 1], x_sem.at[1, d - 1],
                          {X: x_to[d]}) for d in range(1, nx)}
    b_copies = {d: remote(zb_v.at[z_to[d]], inc_v.at[z], b_sem.at[0], b_sem.at[d],
                          {Z: z_to[d]}) for d in range(1, nz)}
    b_to = [remote(zb_v.at[j], inc_v.at[z], b_sem.at[0], b_sem.at[(j + nz - z) % nz], {Z: j})
            for j in range(nz)]
    b_all = remote(zb_v.at[most], inc_v.at[most], b_sem.at[0], b_sem.at[1], other)
    f_copies = {d: remote(inc_v.at[z_from[d]], inc_v.at[z_from[d]], f_sem.at[0],
                          f_sem.at[1], other) for d in range(nz)}
    f_all = remote(inc_v, inc_v, f_sem.at[0], f_sem.at[1], other)

    def step_a(v):
        return v + 1 - 2 * (v % 2)

    def near_of(s, v):
        return jnp.where(s == 0, step_a(v), 3 - v)

    def far_of(s, v):
        return jnp.where(s == 0, 3 - v, step_a(v))

    def columns(block):
        return pl.ds(pl.multiple_of(block * width, width), width)

    parts = 4
    step = DV // 2

    def w_part(s, owner, parity, k):
        far = far_of(s, owner)
        block = (far, near_of(s, far), near_of(s, owner), owner)[k]
        return pl.ds(pl.multiple_of(parity * step, step), step), columns(block)

    near_half, far_half = x % 2, 1 - x % 2

    def wy(s, k):
        to = near_of(s, y)
        rows, cols = w_part(s, to, near_half, k)
        return remote(w_v.at[rows, cols], wn_v.at[s, rows, cols], wy_sem.at[0], wy_sem.at[1 + k],
                      {Y: to})

    def passed(s, k, parity, send, recv, to):
        rows, cols = w_part(s, y, parity, k)
        buf = wn_v.at[s, rows, cols]
        return remote(buf, buf, send, recv, to)

    def wx(s, k):
        return passed(s, k, near_half, wx_sem.at[0], wx_sem.at[1 + k], {X: (x_left, x_right)[s]})

    def wc(s, k):
        return passed(s, k, near_half, wc_sem.at[0], wc_sem.at[1 + k // 2], other)

    def wd(s, k):
        return passed(s, k, far_half, wc_sem.at[0], wc_sem.at[1 + k // 2], other)

    def part_wait(sem, k):
        two = wn_v.at[:, pl.ds(0, step), pl.ds(0, width)]
        remote(two, two, sem.at[0], sem.at[1 + k], other).wait_recv()

    def pass_near(k):
        part_wait(wy_sem, k)
        for s in range(2):
            wx(s, k).start()
            wc(s, k).start()

    def pass_far(k):
        part_wait(wx_sem, k)
        for s in range(2):
            wd(s, k).start()

    def repeat(low, high, f):
        def one(k, _):
            f(k)
            return 0

        lax.fori_loop(low, high, one, 0)

    barrier = pltpu.get_barrier_semaphore()

    def greet(peers):
        for peer in peers:
            pl.semaphore_signal(barrier, inc=1, device_id=peer, device_id_type=MESH_ID)

    greet([other, {Y: y_a}, {Y: y_b}])

    @pl.when(c == 0)
    def _():
        greet([{X: x_left}, {X: x_right}])

    @pl.when(c == 1)
    def _():
        greet([{Z: z_to[d]} for d in range(1, nz)] + [{X: x_to[d]} for d in range(1, nx)])

    loads = []
    for i, (src, dst) in enumerate((
        (g_hbm, g_v), (k_hbm, k_v), (v_hbm, v_v), (w_hbm, w_v), (q_hbm, q_v),
        (og_hbm, og_v), (gain_hbm, gain_v),
    )):
        copy = pltpu.make_async_copy(src, dst, in_sem.at[i])
        copy.start()
        loads.append(copy)
    load_g, load_k, load_v, load_w, load_q, load_og, load_gain = loads

    group = 256
    tri = (
        lax.broadcasted_iota(jnp.int32, (group, group), 0)
        >= lax.broadcasted_iota(jnp.int32, (group, group), 1)
    ).astype(BF16)
    mark("w_g")
    load_g.wait()
    mark("cumsum")
    carry = jnp.zeros((1, DK), F32)
    for h in range(tok // group):
        rows = slice(h * group, (h + 1) * group)
        part = mm(tri, g_v[rows, :]) + carry
        run_v[rows, :] = part
        carry = part[group - 1:group, :]
    total = carry
    es_v[...] = total

    mark("keys")
    load_k.wait()

    def scale_keys(i):
        rows = pl.ds(pl.multiple_of(i * SPAN, SPAN), SPAN)
        kd_v[rows, :] = (k_v[rows, :].astype(F32) * jnp.exp(total - run_v[rows, :])).astype(BF16)

    repeat(0, tok // SPAN, scale_keys)
    mark("state")
    load_v.wait()
    for e in range(2):
        rows = slice(e * half, (e + 1) * half)
        own_v[rows, :] = mm_tn(v_v[:, rows], kd_v[...])
        ss_v[rows, :] = own_v[rows, :].astype(BF16)

    mark("w_barrier")

    @pl.when(c == 0)
    def _():
        pl.semaphore_wait(barrier, 5)
        e_copy.start()
        s_copy.start()
        load_w.wait()
        for k in range(parts):
            for s in range(2):
                wy(s, k).start()
        er_v[...] = jnp.zeros_like(er_v)

    @pl.when(c == 1)
    def _():
        pl.semaphore_wait(barrier, 3 + nz - 1 + nx - 1)

    mark("w_e")

    @pl.when(c == 1)
    def _():
        e_copy.wait_recv()
        lzs_v[...] = total + er_v[...]
        lz_v[z] = lzs_v[...]
        for d in far_first(nz):
            lz_copies[d].start()

    early = er_v[...]
    mark("w_s")

    @pl.when(c == 1)
    def _():
        s_copy.wait_recv()

    mark("chip_state")

    @pl.when(c == 1)
    def _():
        decay = jnp.exp(total)
        for j in range(nz):
            rows = slice(j * piece, (j + 1) * piece)
            zs_v[j] = (own_v[rows, :] + sr_v[rows, :].astype(F32) * decay).astype(BF16)
        for d in far_first(nz):
            z_copies[d].start()
        zr_v[z] = zs_v[z]
        load_w.wait()

    mark("scale_pair")
    load_q.wait()

    def scale_pair(i):
        rows = pl.ds(pl.multiple_of(i * SPAN, SPAN), SPAN)
        r = run_v[rows, :]
        mid = run_v[pl.ds(pl.multiple_of(i * SPAN + SPAN // 2, 8), 1), :]
        q = q_v[rows, :].astype(F32)
        k = k_v[rows, :].astype(F32)
        qa_v[rows, :] = (q * jnp.exp(r - mid)).astype(BF16)
        ka_v[rows, :] = (k * jnp.exp(mid - r)).astype(BF16)
        q0_v[rows, :] = (q * jnp.exp(r)).astype(BF16)
        qp_v[rows, :] = (q * jnp.exp(r + early)).astype(BF16)

    repeat(0, tok // SPAN, scale_pair)

    mark("scale_cross")
    for h, ref in ((SPAN, b_v), (2 * SPAN, c_v), (4 * SPAN, d_v)):
        for start in range(0, tok, 2 * h):
            edge = run_v[start + h - 1:start + h, :]

            def scale_cross(i, start=start, h=h, ref=ref, edge=edge):
                ke = pl.ds(pl.multiple_of(start + i * SPAN, SPAN), SPAN)
                qe = pl.ds(pl.multiple_of(start + h + i * SPAN, SPAN), SPAN)
                ref[ke, :] = (k_v[ke, :].astype(F32) * jnp.exp(edge - run_v[ke, :])).astype(BF16)
                ref[qe, :] = (q_v[qe, :].astype(F32) * jnp.exp(run_v[qe, :] - edge)).astype(BF16)

            repeat(0, h // SPAN, scale_cross)

    mark("attn")
    wide = 2 * SPAN
    ti = lax.broadcasted_iota(jnp.int32, (wide, wide), 0)
    si = lax.broadcasted_iota(jnp.int32, (wide, wide), 1)
    same = (ti // SPAN) == (si // SPAN)
    causal = same & (ti >= si)
    across = (ti // SPAN) > (si // SPAN)
    for m in range(tok // wide):
        rows = slice(m * wide, (m + 1) * wide)
        inside = mm_nt(qa_v[rows, :], ka_v[rows, :])
        between = mm_nt(b_v[rows, :], b_v[rows, :])
        diag = jnp.where(causal, inside, jnp.where(across, between, 0.0)).astype(BF16)
        if m % 2 == 0:
            wgt_v[rows, 0:wide] = diag
            wgt_v[rows, wide:2 * wide] = jnp.zeros_like(diag)
        else:
            before = slice((m - 1) * wide, m * wide)
            wgt_v[rows, 0:wide] = mm_nt(c_v[rows, :], c_v[before, :]).astype(BF16)
            wgt_v[rows, wide:2 * wide] = diag
    wd_v[...] = mm_nt(d_v[group:2 * group, :], d_v[0:group, :]).astype(BF16)
    for h in range(2):
        rows = slice(h * group, (h + 1) * group)
        acc = mm(wgt_v[rows, :], v_v[rows, :])
        if h:
            acc = acc + mm(wd_v[...], v_v[0:group, :])
        loc_v[rows, :] = acc

    @pl.when(c == 1)
    def _():
        for h in range(2):
            rows = slice(h * group, (h + 1) * group)
            loc_v[rows, :] = loc_v[rows, :] + mm_nt(q0_v[rows, :], sr_v[...])

    mark("gate")
    load_og.wait()
    load_gain.wait()

    def gate_rows(i):
        rows = pl.ds(pl.multiple_of(i * SPAN, SPAN), SPAN)
        u = og_v[rows, :].astype(F32)
        gate_v[rows, :] = gain_v[...] * (u / (1.0 + jnp.exp(-u)))

    repeat(0, tok // SPAN, gate_rows)

    mark("w_lz")

    @pl.when(c == 1)
    def _():
        lz_all.wait_recv()
        slab = lz_v[0]
        for j in range(1, nz):
            slab = slab + lz_v[j]
        lxs_v[...] = slab
        for d in range(1, nx):
            pl.when(x + d < nx)(lx_copies[d].start)

        z_all.wait_recv()

        run = jnp.zeros((piece, DK), F32)
        for j in range(nz):
            pre_v[j] = run
            run = run * jnp.exp(lz_v[j]) + zr_v[j].astype(F32)
        xs_v[...] = run.astype(BF16)
        pl.when(x == 0)(x_copies[1].start)
        for d in far_first(nx):
            pl.when((x + d < nx) & ((x > 0) | (d > 1)))(x_copies[d].start)

        for d in range(1, nx):
            pl.when(x >= d)(lx_copies[d].wait_recv)
        for d in near_first(nx):
            pl.when(x >= d)(x_copies[d].wait_recv)

        ent_v[...] = jnp.zeros_like(ent_v)
        for j in range(nx - 1):
            @pl.when(j < x)
            def _(j=j):
                ent_v[...] = ent_v[...] * jnp.exp(lx_v[j]) + xr_v[j].astype(F32)
        enter = ent_v[...]
        log = jnp.zeros((1, DK), F32)
        for j in range(nz):
            zb_v[j] = (pre_v[j] + enter * jnp.exp(log)).astype(BF16)
            log = log + lz_v[j]
        for j in range(nz):
            pl.when(z != j)(b_to[j].start)
        inc_v[z] = zb_v[z]
        f_copies[0].start()

        for d in near_first(nz):
            b_copies[d].wait_recv()
            f_copies[d].start()

    mark("weights")
    ahead = 2

    @pl.when(c == 0)
    def _():
        for k in range(parts):
            pass_near(k)
            if k >= ahead:
                pass_far(k - ahead)

    mark("w_f")

    @pl.when(c == 0)
    def _():
        f_all.wait_recv()

    mark("gated")
    side_tok = tok // 2
    chunks = side_tok // 2 // SPAN
    order = [(s, j) for j in range(chunks) for s in (1, 0)]

    def start_row(s, own, j):
        lead = jnp.where(s == 0, ((y + 1) // 2) % 2, y // 2)
        lead = lead if own else 1 - lead
        return pl.multiple_of(s * side_tok + lead * (side_tok // 2) + j * SPAN, SPAN)

    def gated_rows(s, own, j):
        rows = pl.ds(start_row(s, own, j), SPAN)
        att = loc_v[rows, :] + mm_nt(qp_v[rows, :], inc_v[...].reshape(DV, DK))
        spread = jnp.mean(att * att, axis=-1, keepdims=True)
        return (att * lax.rsqrt(spread + 1e-05) * gate_v[rows, :]).astype(BF16)

    g_copies, r_copies, n_copies = [], [], []
    for s, j in order:
        gs_v[s, j] = gated_rows(s, False, j)
        g_copies.append(remote(gs_v.at[s, j], gr_v.at[s, j], g_sem.at[chunks * 2],
                               g_sem.at[s * chunks + j], {Y: near_of(s, y)}))
        g_copies[-1].start()
        r_copies.append(remote(rs_v.at[s, j], rr_v.at[s, j], r_sem.at[chunks * 2],
                               r_sem.at[s * chunks + j], {Y: far_of(s, y)}))
        n_copies.append(remote(fs_v.at[s, j], fr_v.at[s, j], n_sem.at[chunks * 2],
                               n_sem.at[s * chunks + j], {Y: near_of(s, y)}))
    for s, j in order:
        gm_v[s, j] = gated_rows(s, True, j)

    mark("w_weights")

    def arrive(i):
        both = wn_v.at[0]
        remote(both, both, wc_sem.at[0], wc_sem.at[1 + i], other).wait_recv()

    @pl.when(c == 1)
    def _():
        arrive(0)

    mark("proj")

    def pair_sum(s, j, block):
        cols = columns(block)
        return mm(gm_v[s, j], w_v[:, cols]) + mm(gr_v[s, j], wn_v[s, :, cols])

    for i, (s, j) in enumerate(order):
        far = far_of(s, y)
        mark(f"w_gather{i}")
        g_copies[i].wait_recv()
        mark(f"proj{i}")
        rs_v[s, j, 0] = pair_sum(s, j, far).astype(BF16)
        rs_v[s, j, 1] = pair_sum(s, j, near_of(s, far)).astype(BF16)
        r_copies[i].start()
        if i < ahead:
            mark(f"w_far{i}")

            @pl.when(c == 0)
            def _(i=i):
                pass_far(parts - ahead + i)

    mark("w_weights2")

    @pl.when(c == 1)
    def _():
        arrive(1)

    mark("keep")
    for s, j in order:
        k1_v[s, j] = pair_sum(s, j, near_of(s, y))
        k0_v[s, j] = pair_sum(s, j, y)
    mark("sum")

    for i, (s, j) in enumerate(order):
        mark(f"w_r{i}")
        r_copies[i].wait_recv()
        mark(f"sum{i}")
        fs_v[s, j] = (k1_v[s, j] + rr_v[s, j, 1].astype(F32)).astype(BF16)
        pl.when(c == 0)(n_copies[i].start)
        out_ref[pl.ds(start_row(s, True, j), SPAN), :] = (
            k0_v[s, j] + rr_v[s, j, 0].astype(F32)
        ).astype(BF16)
    mark("last")

    @pl.when(c == 1)
    def _():
        for copy in n_copies:
            copy.start()

    for i, (s, j) in enumerate(order):
        mark(f"w_n{i}")
        n_copies[i].wait_recv()
        out_ref[pl.ds(start_row(s, False, j), SPAN), :] = fr_v[s, j]

    mark("drain")

    @pl.when(c == 0)
    def _():
        e_copy.wait_send()
        s_copy.wait_send()

        one = wn_v.at[0]
        for sem in (wy_sem, wx_sem):
            remote(one, one, sem.at[0], sem.at[1], other).wait_send()
        remote(wn_v, wn_v, wc_sem.at[0], wc_sem.at[1], other).wait_send()

    @pl.when(c == 1)
    def _():
        for copy in (lz_all, z_all, b_all, f_all):
            copy.wait_send()
        for d in range(1, nx):
            pl.when(x + d < nx)(lx_copies[d].wait_send)
            pl.when(x + d < nx)(x_copies[d].wait_send)

    for buf, sem in ((gs_v, g_sem), (rs_v, r_sem), (fs_v, n_sem)):
        remote(buf, buf, sem.at[chunks * 2], sem.at[0], other).wait_send()
    mark(None)


def shards(nx, nz, queries, key_vectors, values, log_gate, out_gate, norm_gain, out_weight):
    tok = queries.shape[0]
    width = out_weight.shape[1] // 4
    piece = DV // nz
    chunks = tok // 4 // SPAN
    any_spec = pl.BlockSpec(memory_space=pl.ANY)
    vmem, dma = pltpu.VMEM, pltpu.SemaphoreType.DMA
    row = (tok, DK)
    weights = vmem(out_weight.shape, BF16)
    blocks = (2, chunks, SPAN, width)
    scratch = [
        vmem(row, BF16), vmem(row, BF16), vmem((tok, DV), BF16), vmem(row, BF16),
        vmem((tok, DV), BF16), vmem((1, DV), F32), weights, vmem((2,) + out_weight.shape, BF16),
        vmem(row, F32), vmem(row, BF16), vmem(row, BF16), vmem(row, BF16), vmem(row, BF16),
        vmem(row, BF16), vmem(row, BF16), vmem(row, BF16), vmem(row, BF16),
        vmem((tok, 256), BF16), vmem((256, 256), BF16), vmem((tok, DV), F32), vmem((tok, DV), F32),
        vmem((1, DK), F32), vmem((1, DK), F32),
        vmem((DV, DK), BF16), vmem((DV, DK), BF16), vmem((DV, DK), F32),
        vmem((1, DK), F32), vmem((nz, 1, DK), F32),
        vmem((nz, piece, DK), BF16), vmem((nz, piece, DK), BF16), vmem((nz, piece, DK), F32),
        vmem((1, DK), F32), vmem((nx, 1, DK), F32),
        vmem((piece, DK), BF16), vmem((nx, piece, DK), BF16), vmem((piece, DK), F32),
        vmem((nz, piece, DK), BF16), vmem((nz, piece, DK), BF16),
        vmem(blocks, BF16), vmem(blocks, BF16), vmem(blocks, BF16),
        vmem((2, chunks, 2, SPAN, width), BF16), vmem((2, chunks, 2, SPAN, width), BF16),
        vmem(blocks, F32), vmem(blocks, F32),
        vmem(blocks, BF16), vmem(blocks, BF16),
        dma((7,)), dma((2,)), dma((2,)), dma((2,)), dma((2,)),
        dma((2, nx - 1)), dma((2, nx - 1)), dma((nz,)), dma((2,)),
        dma((5,)), dma((5,)), dma((3,)),
        dma((2 * chunks + 1,)), dma((2 * chunks + 1,)), dma((2 * chunks + 1,)),
    ]
    return pl.pallas_call(
        functools.partial(body, nx, nz, tok, width),
        out_shape=jax.ShapeDtypeStruct((tok, width), BF16),
        in_specs=[any_spec] * 7,
        out_specs=pl.BlockSpec(memory_space=pltpu.VMEM),
        scratch_shapes=scratch,
        compiler_params=pltpu.CompilerParams(
            collective_id=0, has_side_effects=True, vmem_limit_bytes=40 * 2**20
        ),
    )(*[pltpu.with_memory_space_constraint(v, pltpu.HBM) for v in (
        queries, key_vectors, values, log_gate, out_gate, norm_gain.reshape(1, DV), out_weight)])


def build(devices, nx, nz):
    split = Mesh(devices.reshape(nx, nz, 2, 4), (X, Z, C, Y))
    in_specs = (P(SEQ, Y),) * 5 + (P(Y), P(Y, None))
    return jax.shard_map(
        functools.partial(shards, nx, nz),
        mesh=split, in_specs=in_specs, out_specs=P(SEQ, Y), check_vma=False,
    )


def solution(mesh):
    return build(mesh.devices, 4, mesh.shape["seq"] // 8)
```
